32 devices in a mesh: pw: 16 (over z, x, core), ka: 2 (over y).
Axes of the slice: x: 2, y: 2, z: 4, core: 2. Of those that a mesh axis runs over, the one named last changes fastest.
Arguments:
- waves: bfloat16 [2, 2, 32768, 256], P('ka', None, 'pw'), may hold values from -0.125 to 0.125
- projectors: bfloat16 [2, 2, 32768, 2304], P('ka', None, 'pw'), may hold values from -0.125 to 0.125
- projector_order: int32 [2304], replicated, may hold values from 0 to 2303, each once
- shift_map: int32 [32768], P('pw'), may hold values from 0 to 32767, as said below
- charges: float32 [128, 18, 18], replicated, may hold values from -0.125 to 0.125
- atom_phase: float32 [128], replicated, may hold values from -3.140625 to 3.140625
Outputs:
- margins: float32 [2, 256, 2, 256], P('ka', 'pw')
The draws below stay inside these ranges and needn't reach their ends.
Inputs may be any that keep to these rules, and one draw needn't show every extreme that they name: `projector_order`: each projector slot once. `shift_map`: a permutation of the plane waves that maps every aligned block of 2048 plane waves onto itself.
All inputs are finite; a program needn't handle non-finite values.
Results may differ from the reference program's by a relative error of at most 0.0003.
Values may be sent and summed in bfloat16 or wider, within the bound.
A program may use at most 128 MiB of HBM per device.

```python
import jax
import jax.numpy as jnp
from jax import lax

NB = 256
PPA = 18
PW_DEV = 2048
KPTS = 2
NPW = 32768
ATOMS = 128
NPROJ = 2304


def draw_shift_map(key, part):
    blocks = NPW // PW_DEV
    keys = jax.random.split(key, blocks)
    perms = jax.vmap(lambda single: jax.random.permutation(single, PW_DEV))(keys)
    offsets = (jnp.arange(blocks, dtype=jnp.int32) * PW_DEV)[:, None]
    return (perms.astype(jnp.int32) + offsets).reshape(-1).astype(jnp.int32)


def level_of(rng, extent, shards, low, high):
    def one(position, parts):
        steps = jax.random.uniform(jax.random.fold_in(jax.random.fold_in(rng, 6), position), (parts,), jnp.float32, low / len(shards), high / len(shards))
        return jnp.repeat(jnp.exp(steps), extent[position] // parts).reshape((-1,) + (1,) * (len(extent) - position - 1))

    gain = one(*shards[0])
    for cut in shards[1:]:
        gain = gain * one(*cut)
    return gain


def gaussian(key, dims, width, reach, cuts=(), kind=jnp.bfloat16):
    factor_of = level_of(key, dims, cuts, -0.22, 0.18) if cuts else 1.0
    array = jax.random.normal(key, dims, jnp.float32) * width * factor_of
    return jnp.minimum(jnp.maximum(array, -reach), reach).astype(kind)


def setup_inputs(seed: int = 0) -> dict:
    seeds = jax.random.split(jax.random.key(seed), 7)
    waves = gaussian(seeds[0], (KPTS, 2, NPW, NB), (NPW // 16) ** -0.5, 0.125, ((0, 2), (2, 16)))
    projectors = gaussian(seeds[1], (KPTS, 2, NPW, NPROJ), (NPW // 16) ** -0.5, 0.125, ((0, 2), (2, 16)))
    projector_order = jax.random.permutation(seeds[2], NPROJ).astype(jnp.int32)
    shift_map = draw_shift_map(jax.random.fold_in(seeds[6], 71), 0)
    charges = gaussian(seeds[4], (ATOMS, PPA, PPA), NPROJ ** -0.5, 0.125, (), jnp.float32)
    atom_phase = jnp.clip(jax.random.uniform(seeds[5], (ATOMS,), jnp.float32, -3.140625, 3.140625), -3.140625, 3.140625)
    return {"waves": waves, "projectors": projectors, "projector_order": projector_order, "shift_map": shift_map, "charges": charges, "atom_phase": atom_phase}


def contract(left, right, precision=None):
    return lax.dot_general(left, right, (((0,), (0,)), ((), ())), precision=precision, preferred_element_type=jnp.float32)


def complex_cross(left, right, precision=None):
    real = contract(left[0], right[0], precision) + contract(left[1], right[1], precision)
    imag = contract(left[0], right[1], precision) - contract(left[1], right[0], precision)
    return jnp.stack([real, imag], axis=1)


def reference(waves, projectors, projector_order, shift_map, charges, atom_phase):
    inverse = jnp.argsort(projector_order).astype(jnp.int32)
    sym = 0.5 * (charges + jnp.transpose(charges, (0, 2, 1)))

    def project(pair):
        wave, beta = pair
        real = contract(beta[0], wave[0]) + contract(beta[1], wave[1])
        imag = contract(beta[0], wave[1]) - contract(beta[1], wave[0])
        return jnp.stack([real, imag])[:, inverse, :]

    proj = lax.map(project, (waves, projectors))
    last_wave = waves[0][:, shift_map.astype(jnp.int32), :]
    next_wave = jnp.concatenate([waves[1:], last_wave[None]], axis=0)
    repeated = jnp.repeat(atom_phase, PPA)
    cosine = jnp.cos(repeated)[:, None]
    sine = jnp.sin(repeated)[:, None]
    first = proj[0]
    rotated = jnp.stack([first[0] * cosine + first[1] * sine, first[1] * cosine - first[0] * sine])
    next_proj = jnp.concatenate([proj[1:], rotated[None]], axis=0)

    def margin(items):
        wave, nwave, pk, pn = items
        plane = complex_cross(wave, nwave)
        split = pn.reshape(2, ATOMS, PPA, NB)
        weighted = jnp.einsum("apq,raqj->rapj", sym, split, precision=lax.Precision.HIGHEST).reshape(2, NPROJ, NB)
        aug = complex_cross(pk, weighted, lax.Precision.HIGHEST)
        return plane + aug

    return lax.map(margin, (waves, next_wave, proj, next_proj))
```

```python
import functools

import jax
import jax.numpy as jnp
from jax import lax
from jax.experimental import pallas as pl
from jax.experimental.pallas import tpu as pltpu
from jax.sharding import PartitionSpec as P

MESH = pl.DeviceIdType.MESH
LANES = 128
TOP = 32767.0
HIGH = lax.Precision.HIGHEST


def dot(left, right, dims, precision=None):
    return lax.dot_general(
        left, right, (((dims[0],), (dims[1],)), ((), ())),
        precision=precision, preferred_element_type=jnp.float32,
    )


def contract(left, right, precision=None):
    return dot(left, right, (0, 0), precision)


def cross(left, right):
    real = contract(left[0], right[0]) + contract(left[1], right[1])
    imag = contract(left[0], right[1]) - contract(left[1], right[0])
    return real, imag


def low(v):
    return jnp.right_shift(jnp.left_shift(v, 16), 16).astype(jnp.float32)


def high(v):
    return jnp.right_shift(v, 16).astype(jnp.float32)


def code(x, inv):
    return jnp.floor(x * inv + 0.5).astype(jnp.int32)


def pack(real, imag, inv_real, inv_imag):
    return jnp.bitwise_or(
        jnp.left_shift(code(imag, inv_imag), 16),
        jnp.bitwise_and(code(real, inv_real), 0xFFFF),
    )


def fold(x):
    return jnp.max(jnp.abs(x).reshape(x.shape[0] // 8, 8, x.shape[1]), axis=0)


def scale_of(top):
    return jnp.maximum(jnp.max(top, axis=0, keepdims=True), 1e-30) * (1.0 / TOP)


def block_of(size):
    for block in (512, 256, 128):
        if size % block == 0:
            return block
    return size


def fused_kernel(
    n, kn, ppa, order_hbm, shift_hbm, phase_hbm, charge_hbm, wave_hbm, beta_hbm, out,
    order, shift, phase, charge, inv_v, inv_s, spread, sym, wave, beta, rhs, proj_t, top, inv_b, packed,
    gs, go, cr, sc0, sc0_r, xf, xs, xr, scx, scx_r, acc, zs, zr, scz, scz_r, mine, ys, yr, scy, scy_r,
    wr, picked, stage, part, ms, mr, scm, scm_r, macc, ds, dr, scd, scd_r,
    local_sems, core_sems, core_scale_sems, x_sems, z_sems, y_sems, wave_sems, m_sems, d_sems,
):
    me = lax.axis_index("pw")
    k = lax.axis_index("ka")
    ahead, behind = lax.rem(k + 1, kn), lax.rem(k + kn - 1, kn)
    last_k = k == kn - 1
    paired = kn == 2
    pw_dev, nb = wave.shape[1], wave.shape[2]
    nproj = beta.shape[2]
    streams = nb // LANES
    rows = gs.shape[2]
    parts = 2 if rows % 16 == 0 else 1
    rs = rows // parts
    halfn, zn = n // 2, n // 4
    share = nb // n
    core, xbit, mez, mej = me & 1, (me >> 1) & 1, me >> 2, me >> 1
    tile = block_of(nproj) if nproj % 256 else 256
    tiles = nproj // tile
    third = wr.shape[2]

    def beta_copy(t):
        at = pl.ds(pl.multiple_of(t * tile, tile), tile)
        return pltpu.make_async_copy(beta_hbm.at[0, :, :, at], beta.at[:, :, at], local_sems.at[t])

    small = [
        pltpu.make_async_copy(src, dst, local_sems.at[tiles + i])
        for i, (src, dst) in enumerate((
            (order_hbm, order), (wave_hbm.at[0], wave), (shift_hbm, shift), (phase_hbm, phase),
            (charge_hbm, charge.at[:, pl.ds(0, ppa), :]), (inv_v, inv_s),
        ))
    ]
    for copy in small[:2]:
        copy.start()
    for t in range(tiles):
        beta_copy(t).start()
    for copy in small[2:5]:
        copy.start()

    barrier = pltpu.get_barrier_semaphore()
    greet = [{"pw": me ^ 1}] + [{"pw": me ^ (d << 1)} for d in range(1, halfn)]
    if paired:
        greet += [{"ka": ahead, "pw": me ^ (d << 1)} for d in range(halfn)]
    else:
        greet += [{"ka": ahead}, {"ka": behind}]
    for where in greet:
        pl.semaphore_signal(barrier, inc=1, device_id=where, device_id_type=MESH)

    def remote(src, dst, send, recv, where):
        return pltpu.make_async_remote_copy(
            src_ref=src, dst_ref=dst, send_sem=send, recv_sem=recv,
            device_id=where, device_id_type=MESH,
        )

    def invert():
        blocks = inv_v.shape[0]
        small[0].wait()
        slots = order[...]
        upper, lower = jnp.right_shift(slots, 7), jnp.bitwise_and(slots, 127)
        place = lax.broadcasted_iota(jnp.int32, (1, nproj), 1)
        hot_u = lax.broadcasted_iota(jnp.int32, (blocks, nproj), 0) == upper
        hot_l = lax.broadcasted_iota(jnp.int32, (LANES, nproj), 0) == lower
        coarse = jnp.right_shift(place, 4).astype(jnp.float32)
        fine = jnp.bitwise_and(place, 15).astype(jnp.float32)
        left = jnp.concatenate([jnp.where(hot_u, coarse, 0.0), jnp.where(hot_u, fine, 0.0)], axis=0)
        found = dot(left.astype(jnp.bfloat16), jnp.where(hot_l, 1.0, 0.0).astype(jnp.bfloat16), (1, 1))
        found = (found[:blocks] * 16.0 + found[blocks:] + 0.5).astype(jnp.int32)
        inv_v[...] = jnp.clip(found, 0, nproj - 1)
        small[5].start()

    def transpose_waves():
        small[1].wait()
        for p in range(2):
            flat = wave[p].T
            for h in range(streams):
                mid = flat[h * LANES : (h + 1) * LANES]
                rhs[h, p, :LANES, :] = mid
                rhs[h, 1 - p, LANES:, :] = mid if p else -mid

    def multiply(h):
        top[...] = jnp.zeros_like(top)

        def step(t, carry):
            if h == 0:
                beta_copy(t).wait()
            at = pl.ds(pl.multiple_of(t * tile, tile), tile)
            got = dot(rhs[h, 0], beta[0, :, at], (1, 0)) + dot(rhs[h, 1], beta[1, :, at], (1, 0))
            proj_t[:, at] = got
            peak = top[...]
            for b in range(tile // LANES):
                peak = jnp.maximum(peak, jnp.abs(got[:, b * LANES : (b + 1) * LANES]))
            top[...] = peak
            return carry

        lax.fori_loop(0, tiles, step, 0)

    def encode(h):
        peak = jnp.max(top[...], axis=1, keepdims=True)
        scale = jnp.maximum(peak, 1e-30) * (1.0 / TOP)
        inv_b[...] = jnp.broadcast_to(1.0 / scale, inv_b.shape)
        flat = jnp.broadcast_to(scale, inv_b.shape)
        sc0[h, 0:1, :] = flat[:LANES].T[0:1]
        sc0[h, 1:2, :] = flat[LANES:].T[0:1]

        def step(t, carry):
            at = pl.ds(pl.multiple_of(t * LANES, LANES), LANES)
            coded = pack(proj_t[:LANES, at], proj_t[LANES:, at], inv_b[:LANES], inv_b[LANES:])
            packed[at, :] = coded.T
            return carry

        lax.fori_loop(0, nproj // LANES, step, 0)

    def gather(dst, h, parity, sub):
        def one(j, carry):
            base = ((j << 1) | parity) * rows + sub * rs
            for g in range(rs // 8):
                slot = base + 8 * g
                upper, lower = slot >> 7, slot & 127
                taken = [packed[pl.ds(inv_s[upper, lower + r], 1), :] for r in range(8)]
                dst[h, j, pl.ds(sub * rs + 8 * g, 8), :] = jnp.concatenate(taken, axis=0)
            return carry

        lax.fori_loop(0, halfn, one, 0)

    def span(sub):
        return pl.ds(sub * rs, rs)

    def core_copy(h, sub):
        return remote(
            gs.at[h, :, span(sub)], cr.at[h, :, span(sub)],
            core_sems.at[0, h, sub], core_sems.at[1, h, sub], {"pw": me ^ 1},
        )

    def core_scale_copy(h):
        return remote(sc0.at[h], sc0_r.at[h], core_scale_sems.at[0, h], core_scale_sems.at[1, h], {"pw": me ^ 1})

    def x_copies(h, sub):
        sems, where = x_sems, {"pw": me ^ 2}
        return [
            remote(xs.at[h, :, span(sub)], xr.at[h, :, span(sub)], sems.at[0, h, sub, 0], sems.at[1, h, sub, 0], where),
            remote(scx.at[h, sub], scx_r.at[h, sub], sems.at[0, h, sub, 1], sems.at[1, h, sub, 1], where),
        ]

    def z_copies(h, sub):
        made = []
        for d in range(1, zn):
            where = {"pw": me ^ (d << 2)}
            made.append(remote(
                zs.at[h, d - 1, span(sub)], zr.at[h, d - 1, span(sub)],
                z_sems.at[0, h, sub, d - 1, 0], z_sems.at[1, h, sub, d - 1, 0], where,
            ))
            made.append(remote(
                scz.at[h, sub], scz_r.at[h, sub, d - 1],
                z_sems.at[0, h, sub, d - 1, 1], z_sems.at[1, h, sub, d - 1, 1], where,
            ))
        return made

    def y_copies(h, sub):
        where = {"ka": behind}
        return [
            remote(ys.at[h, span(sub)], yr.at[h, span(sub)], y_sems.at[0, h, sub, 0], y_sems.at[1, h, sub, 0], where),
            remote(scy.at[h, sub], scy_r.at[h, sub], y_sems.at[0, h, sub, 1], y_sems.at[1, h, sub, 1], where),
        ]

    none = jnp.zeros((8, LANES), jnp.float32)

    def put_scale(ref, h, sub, tops):
        scales = [scale_of(t) for t in tops]
        ref[h, sub, 0:1, :] = scales[0]
        ref[h, sub, 1:2, :] = scales[1]
        return [1.0 / s for s in scales]

    def send_core(h, sub):
        gather(gs, h, 1 - core, sub)
        if sub == 0:
            core_scale_copy(h).start()
        core_copy(h, sub).start()

    def step_core(h, sub):
        if sub == 0:
            core_scale_copy(h).wait()
        core_copy(h, sub).wait()
        at = span(sub)
        own_r, own_i = sc0[h, 0:1, :], sc0[h, 1:2, :]
        sib_r, sib_i = sc0_r[h, 0:1, :], sc0_r[h, 1:2, :]

        def total(j):
            a, b = go[h, j, at, :], cr[h, j, at, :]
            return low(a) * own_r + low(b) * sib_r, high(a) * own_i + high(b) * sib_i

        def first(z, carry):
            tr, ti = carry
            real, imag = total((z << 1) | (1 - xbit))
            xf[z, 0], xf[z, 1] = real, imag
            return jnp.maximum(tr, fold(real)), jnp.maximum(ti, fold(imag))

        inv = put_scale(scx, h, sub, lax.fori_loop(0, zn, first, (none, none)))

        def second(z, carry):
            xs[h, z, at, :] = pack(xf[z, 0], xf[z, 1], *inv)
            return carry

        lax.fori_loop(0, zn, second, 0)
        for copy in x_copies(h, sub):
            copy.start()

        def keep(z, carry):
            real, imag = total((z << 1) | xbit)
            acc[h, z, 0, at, :] = real
            acc[h, z, 1, at, :] = imag
            return carry

        lax.fori_loop(0, zn, keep, 0)

    def step_x(h, sub):
        for copy in x_copies(h, sub):
            copy.wait()
        at = span(sub)
        s_r, s_i = scx_r[h, sub, 0:1, :], scx_r[h, sub, 1:2, :]

        def total(z):
            v = xr[h, z, at, :]
            real = acc[h, z, 0, at, :] + low(v) * s_r
            imag = acc[h, z, 1, at, :] + high(v) * s_i
            acc[h, z, 0, at, :] = real
            acc[h, z, 1, at, :] = imag
            return real, imag

        def first(d, carry):
            tr, ti = carry
            real, imag = total(mez ^ d)
            return jnp.maximum(tr, fold(real)), jnp.maximum(ti, fold(imag))

        inv = put_scale(scz, h, sub, lax.fori_loop(1, zn, first, (none, none)))

        def second(d, carry):
            z = mez ^ d
            zs[h, d - 1, at, :] = pack(acc[h, z, 0, at, :], acc[h, z, 1, at, :], *inv)
            return carry

        lax.fori_loop(1, zn, second, 0)
        for copy in z_copies(h, sub):
            copy.start()
        total(mez)

    def step_z(h, sub):
        for copy in z_copies(h, sub):
            copy.wait()
        at = span(sub)
        real, imag = acc[h, mez, 0, at, :], acc[h, mez, 1, at, :]
        for d in range(zn - 1):
            v = zr[h, d, at, :]
            real = real + low(v) * scz_r[h, sub, d, 0:1, :]
            imag = imag + high(v) * scz_r[h, sub, d, 1:2, :]
        cols = slice(h * LANES, (h + 1) * LANES)
        mine[0, at, cols] = real
        mine[1, at, cols] = imag
        inv = put_scale(scy, h, sub, (fold(real), fold(imag)))
        ys[h, at, :] = pack(real, imag, *inv)
        for copy in y_copies(h, sub):
            copy.start()

    def wave_copy(i, src):
        return remote(src, wr.at[i], wave_sems.at[0, i], wave_sems.at[1, i], {"ka": behind})

    def own_rows(i):
        return wave_hbm.at[0, :, pl.ds(i * third, third), :]

    def send_waves():
        if not paired:
            wave_copy(0, wave_hbm.at[0]).start()
            return

        @pl.when(k == 0)
        def _():
            wave_copy(0, own_rows(3)).start()

        @pl.when(k == 1)
        def _():
            for i in range(3):
                wave_copy(i, own_rows(i)).start()

    def spread_shift():
        small[2].wait()
        for b in range(pw_dev // LANES):
            line = shift[0:1, b * LANES : (b + 1) * LANES] - me * pw_dev
            spread[pl.ds(b * LANES, LANES), :] = jnp.broadcast_to(line, (LANES, LANES)).T

    def permute(dst, src, start, size, offset):
        block = min(block_of(size), 256)

        def step(b, carry):
            at = pl.ds(pl.multiple_of(start + b * block, block), block)
            to = pl.ds(pl.multiple_of(offset + b * block, block), block)
            want = spread[at, :]
            lane = lax.broadcasted_iota(jnp.int32, (block, LANES), 1)
            hot = jnp.concatenate(
                [jnp.where(want == lane + g * LANES, 1.0, 0.0) for g in range(pw_dev // LANES)], axis=1
            ).astype(jnp.bfloat16)
            for p in range(2):
                dst[p, to, :] = dot(hot, src(p), (1, 0)).astype(jnp.bfloat16)
            return carry

        lax.fori_loop(0, size // block, step, 0)

    def send_picked():
        @pl.when(k == 0)
        def _():
            permute(stage, lambda p: wave[p], 3 * third, third, 0)
            wave_copy(1, stage).start()

    def build_picked():
        @pl.when(k == 0)
        def _():
            permute(picked, lambda p: wave[p], 0, 3 * third, 0)

    def add(which, values, fresh):
        for c in range(2):
            if fresh:
                part[which, c] = values[c]
            else:
                part[which, c] += values[c]

    def piece(ref, i):
        return [ref[p, i * third : (i + 1) * third, :] for p in range(2)]

    def plane_first(i):
        @pl.when(k == 0)
        def _():
            wave_copy(i, own_rows(i)).wait_recv()
            got = [wr[i, 0], wr[i, 1]]
            add(0, cross(piece(wave, i), got), i == 0)
            add(1, cross(got, piece(picked, i)), i == 0)

    def plane_second(i):
        @pl.when(k == 1)
        def _():
            wave_copy(i, own_rows(i)).wait_recv()
            got = [wr[i, 0], wr[i, 1]]
            if i == 0:
                add(1, cross(got, piece(wave, 3)), True)
            else:
                add(0, cross(piece(wave, 3), got), True)

    def drain_waves():
        if not paired:
            wave_copy(0, wave_hbm.at[0]).wait_send()
            return

        @pl.when(k == 0)
        def _():
            wave_copy(0, own_rows(3)).wait_send()
            wave_copy(1, stage).wait_send()

        @pl.when(k == 1)
        def _():
            for i in range(3):
                wave_copy(i, own_rows(i)).wait_send()

    def plane_ring():
        wave_copy(0, wave_hbm.at[0]).wait_recv()

        @pl.when(last_k)
        def _():
            permute(picked, lambda p: wr[0, p], 0, pw_dev, 0)

        @pl.when(k != kn - 1)
        def _():
            picked[...] = wr[0]

        add(0, cross([wave[0], wave[1]], [picked[0], picked[1]]), True)

    def make_tables():
        small[3].wait()
        small[4].wait()
        atoms = phase.shape[1]
        own_atoms = rows // ppa
        row_i = lax.broadcasted_iota(jnp.int32, (rows, atoms), 0)
        lane = lax.broadcasted_iota(jnp.int32, (rows, atoms), 1)
        away = row_i - ppa * (lane - me * own_atoms)
        hit = (away >= 0) & (away < ppa)
        angle = jnp.where(last_k, phase[...], 0.0)
        cosine = jnp.sum(jnp.where(hit, jnp.cos(angle), 0.0), axis=1, keepdims=True)
        sine = jnp.sum(jnp.where(hit, jnp.sin(angle), 0.0), axis=1, keepdims=True)
        pad = charge.shape[1]
        flat = charge[...].reshape(ppa * pad, atoms)
        pick = jnp.where(hit, 1.0, 0.0)
        every = dot(pick, flat, (1, 1), HIGH)

        def iota(shape, axis):
            return lax.broadcasted_iota(jnp.int32, shape, axis).astype(jnp.float32)

        def div(x, by):
            return jnp.floor((x + 0.5) * (1.0 / by))

        shape = (rows, ppa * pad)
        r, c = iota(shape, 0), iota(shape, 1)
        own_p = r - ppa * div(r, ppa)
        col_p = div(c, pad)
        kept = jnp.where((own_p == col_p) & (c - pad * col_p < ppa), every, 0.0)
        shape = (ppa * pad, rows)
        c, j = iota(shape, 0), iota(shape, 1)
        widen = jnp.where(c - pad * div(c, pad) == j - ppa * div(j, ppa), 1.0, 0.0)
        full = dot(kept, widen, (1, 0), HIGH) + dot(widen, kept, (0, 1), HIGH)
        shape = (rows, rows)
        same = div(iota(shape, 0), ppa) == div(iota(shape, 1), ppa)
        sym[...] = jnp.where(same, 0.5 * full, 0.0)
        return cosine, sine

    def m_copies(w):
        where = {"pw": me ^ 1}
        return [
            remote(ms.at[w], mr.at[w], m_sems.at[0, w, 0], m_sems.at[1, w, 0], where),
            remote(scm.at[w], scm_r.at[w], m_sems.at[0, w, 1], m_sems.at[1, w, 1], where),
        ]

    def d_copies(w):
        made = []
        for d in range(1 - w, halfn):
            where = {"pw": me ^ (d << 1)}
            if w:
                where["ka"] = ahead
            made.append(remote(
                ds.at[w, d], dr.at[w, d], d_sems.at[0, w, d, 0], d_sems.at[1, w, d, 0], where,
            ))
            made.append(remote(
                scd.at[w], scd_r.at[w, d], d_sems.at[0, w, d, 1], d_sems.at[1, w, d, 1], where,
            ))
        return made

    wide = jnp.zeros((8, nb), jnp.float32)

    def block_at(j, parity):
        return pl.ds(pl.multiple_of(((j << 1) | parity) * share, share), share)

    def margin_scale(ref, w, tops):
        scales = [scale_of(t) for t in tops]
        ref[w, 0:1, :] = scales[0]
        ref[w, 1:2, :] = scales[1]
        return [1.0 / s for s in scales]

    def send_margin(w):
        def first(j, carry):
            at = block_at(j, 1 - core)
            return jnp.maximum(carry[0], fold(part[w, 0, at, :])), jnp.maximum(carry[1], fold(part[w, 1, at, :]))

        inv = margin_scale(scm, w, lax.fori_loop(0, halfn, first, (wide, wide)))

        def second(j, carry):
            at = block_at(j, 1 - core)
            ms[w, j] = pack(part[w, 0, at, :], part[w, 1, at, :], *inv)
            return carry

        lax.fori_loop(0, halfn, second, 0)
        for copy in m_copies(w):
            copy.start()

    def step_margin(w):
        for copy in m_copies(w):
            copy.wait()
        s_r, s_i = scm_r[w, 0:1, :], scm_r[w, 1:2, :]

        def first(d, carry):
            j = mej ^ d
            at = block_at(j, core)
            v = mr[w, j]
            real = part[w, 0, at, :] + low(v) * s_r
            imag = part[w, 1, at, :] + high(v) * s_i
            macc[w, d, 0], macc[w, d, 1] = real, imag
            return jnp.maximum(carry[0], fold(real)), jnp.maximum(carry[1], fold(imag))

        inv = margin_scale(scd, w, lax.fori_loop(0, halfn, first, (wide, wide)))

        def second(d, carry):
            ds[w, d] = pack(macc[w, d, 0], macc[w, d, 1], *inv)
            return carry

        lax.fori_loop(1 - w, halfn, second, 0)
        for copy in d_copies(w):
            copy.start()

    def finish_margin(w, real, imag):
        for copy in d_copies(w):
            copy.wait()
        for d in range(1 - w, halfn):
            v = dr[w, d]
            real = real + low(v) * scd_r[w, d, 0:1, :]
            imag = imag + high(v) * scd_r[w, d, 1:2, :]
        return real, imag

    last = streams - 1
    invert()
    transpose_waves()
    pl.semaphore_wait(barrier, len(greet))
    send_waves()
    small[5].wait()
    for h in range(streams):
        multiply(h)
        encode(h)
        for sub in range(parts):
            send_core(h, sub)
        for sub in range(parts):
            gather(go, h, core, sub)
            step_core(h, sub)
            if h > 0:
                step_x(h - 1, sub)
    spread_shift()
    if paired:
        send_picked()
        build_picked()
        plane_first(0)
        plane_second(0)
        plane_first(1)
    cosine, sine = make_tables()
    step_x(last, 0)
    for h in range(last):
        for sub in range(parts):
            step_z(h, sub)
    for sub in range(1, parts):
        step_x(last, sub)
    if paired:
        plane_first(2)
        send_margin(1)
    for sub in range(parts):
        step_z(last, sub)
    if paired:
        step_margin(1)
        plane_second(1)
    else:
        plane_ring()
    for h in range(streams):
        for sub in range(parts):
            for copy in y_copies(h, sub):
                copy.wait()

    def next_part(take, c):
        lines = []
        for sub in range(parts):
            pieces = [take(yr[h, span(sub), :]) * scy_r[h, sub, c : c + 1, :] for h in range(streams)]
            lines.append(jnp.concatenate(pieces, axis=1))
        return jnp.concatenate(lines, axis=0)

    nr, ni = next_part(low, 0), next_part(high, 1)
    turned = jnp.concatenate([nr * cosine + ni * sine, ni * cosine - nr * sine], axis=1)
    weighted = dot(sym[...], turned, (1, 0), HIGH)
    by_real = contract(mine[0], weighted, HIGH)
    by_imag = contract(mine[1], weighted, HIGH)
    part[0, 0] += by_real[:, :nb] + by_imag[:, nb:]
    part[0, 1] += by_real[:, nb:] - by_imag[:, :nb]
    send_margin(0)
    step_margin(0)
    real, imag = macc[0, 0, 0], macc[0, 0, 1]
    if paired:
        real, imag = finish_margin(1, real, imag)
    real, imag = finish_margin(0, real, imag)
    drain_waves()
    out[0] = real
    out[1] = imag


def fused(n, kn, order, shift, phase, charges, waves, projectors):
    pw_dev, nb = waves.shape[2], waves.shape[3]
    nproj = projectors.shape[3]
    atoms = phase.shape[1]
    ppa = charges.shape[0]
    rows, share = nproj // n, nb // n
    h = nb // LANES
    parts = 2 if rows % 16 == 0 else 1
    zn, half = n // 4, n // 2
    pad = -(-ppa // 8) * 8
    blocks = -(-nproj // (8 * LANES)) * 8
    paired = kn == 2
    slots, third = (3, pw_dev // 4) if paired else (1, pw_dev)
    kinds = 2 if paired else 1
    anywhere = pl.BlockSpec(memory_space=pl.ANY)
    f32, i32, bf16 = jnp.float32, jnp.int32, jnp.bfloat16
    tile = block_of(nproj) if nproj % 256 else 256
    scratch = [
        ((1, nproj), i32), ((1, pw_dev), i32), ((1, atoms), f32), ((ppa, pad, atoms), f32),
        ((blocks, LANES), i32), "smem", ((pw_dev, LANES), i32), ((rows, rows), f32),
        ((2, pw_dev, nb), bf16), ((2, pw_dev, nproj), bf16), ((h, 2, 2 * LANES, pw_dev), bf16),
        ((2 * LANES, nproj), f32), ((2 * LANES, LANES), f32), ((2 * LANES, LANES), f32), ((nproj, LANES), i32),
        ((h, half, rows, LANES), i32), ((h, half, rows, LANES), i32), ((h, half, rows, LANES), i32),
        ((h, 2, LANES), f32), ((h, 2, LANES), f32),
        ((zn, 2, rows // parts, LANES), f32), ((h, zn, rows, LANES), i32), ((h, zn, rows, LANES), i32),
        ((h, parts, 2, LANES), f32), ((h, parts, 2, LANES), f32), ((h, zn, 2, rows, LANES), f32),
        ((h, zn - 1, rows, LANES), i32), ((h, zn - 1, rows, LANES), i32),
        ((h, parts, 2, LANES), f32), ((h, parts, zn - 1, 2, LANES), f32), ((2, rows, nb), f32),
        ((h, rows, LANES), i32), ((h, rows, LANES), i32), ((h, parts, 2, LANES), f32), ((h, parts, 2, LANES), f32),
        ((slots, 2, third, nb), bf16), ((2, slots * third, nb), bf16), ((2, third, nb), bf16),
        ((kinds, 2, nb, nb), f32), ((kinds, half, share, nb), i32), ((kinds, half, share, nb), i32),
        ((kinds, 2, nb), f32), ((kinds, 2, nb), f32), ((kinds, half, 2, share, nb), f32),
        ((kinds, half, share, nb), i32), ((kinds, half, share, nb), i32),
        ((kinds, 2, nb), f32), ((kinds, half, 2, nb), f32),
    ]
    made = [pltpu.SMEM((blocks, LANES), i32) if s == "smem" else pltpu.VMEM(*s) for s in scratch]
    sems = [
        (nproj // tile + 6,), (2, h, parts), (2, h), (2, h, parts, 2), (2, h, parts, zn - 1, 2),
        (2, h, parts, 2), (2, slots), (2, kinds, 2), (2, kinds, half, 2),
    ]
    return pl.pallas_call(
        functools.partial(fused_kernel, n, kn, ppa),
        out_shape=jax.ShapeDtypeStruct((2, share, nb), f32),
        in_specs=[anywhere] * 6,
        out_specs=pl.BlockSpec(memory_space=pltpu.VMEM),
        scratch_shapes=made + [pltpu.SemaphoreType.DMA(s) for s in sems],
        compiler_params=pltpu.CompilerParams(
            collective_id=0, has_side_effects=True, vmem_limit_bytes=62 * 2**20
        ),
    )(order, shift, phase, charges, waves, projectors)


def local(waves, projectors, projector_order, shift_map, charges, atom_phase):
    n = lax.axis_size("pw")
    kn = lax.axis_size("ka")
    summed = fused(
        n, kn, projector_order[None, :], shift_map[None, :], atom_phase[None, :],
        jnp.transpose(charges, (1, 2, 0)), waves, projectors,
    )
    return jnp.transpose(summed, (1, 0, 2))[None]


def solution(mesh):
    placed = (P("ka", None, "pw", None), P("ka", None, "pw", None), P(), P("pw"), P(), P())
    return jax.shard_map(
        local, mesh=mesh, in_specs=placed, out_specs=P("ka", "pw", None, None), check_vma=False
    )
```

```python
import functools

import jax
import jax.numpy as jnp
from jax import lax
from jax.experimental import pallas as pl
from jax.experimental.pallas import tpu as pltpu
from jax.sharding import PartitionSpec as P

MESH = pl.DeviceIdType.MESH
LANES = 128
TOP = 32767.0
HIGH = lax.Precision.HIGHEST


def dot(left, right, dims, precision=None):
    return lax.dot_general(
        left, right, (((dims[0],), (dims[1],)), ((), ())),
        precision=precision, preferred_element_type=jnp.float32,
    )


def contract(left, right, precision=None):
    return dot(left, right, (0, 0), precision)


def cross(left, right):
    real = contract(left[0], right[0]) + contract(left[1], right[1])
    imag = contract(left[0], right[1]) - contract(left[1], right[0])
    return real, imag


def low(v):
    return jnp.right_shift(jnp.left_shift(v, 16), 16).astype(jnp.float32)


def high(v):
    return jnp.right_shift(v, 16).astype(jnp.float32)


def code(x, inv):
    return jnp.floor(x * inv + 0.5).astype(jnp.int32)


def pack(real, imag, inv_real, inv_imag):
    return jnp.bitwise_or(
        jnp.left_shift(code(imag, inv_imag), 16),
        jnp.bitwise_and(code(real, inv_real), 0xFFFF),
    )


def fold(x):
    return jnp.max(jnp.abs(x).reshape(x.shape[0] // 8, 8, x.shape[1]), axis=0)


def scale_of(top):
    return jnp.maximum(jnp.max(top, axis=0, keepdims=True), 1e-30) * (1.0 / TOP)


def block_of(size):
    for block in (512, 256, 128):
        if size % block == 0:
            return block
    return size


def fused_kernel(
    n, kn, ppa, order_hbm, shift_hbm, phase_hbm, charge_hbm, wave_hbm, beta_hbm, out,
    order, shift, phase, charge, inv_v, inv_s, spread, sym, wave, beta, rhs, proj_t, top, inv_b, packed,
    gs, go, cr, sc0, sc0_r, xf, xs, xr, scx, scx_r, acc, zs, zr, scz, scz_r, mine, ys, yr, scy, scy_r,
    wr, picked, stage, part, ms, mr, scm, scm_r, macc, ds, dr, scd, scd_r,
    local_sems, core_sems, core_scale_sems, x_sems, z_sems, y_sems, wave_sems, m_sems, d_sems,
):
    me = lax.axis_index("pw")
    k = lax.axis_index("ka")
    ahead, behind = lax.rem(k + 1, kn), lax.rem(k + kn - 1, kn)
    last_k = k == kn - 1
    paired = kn == 2
    pw_dev, nb = wave.shape[1], wave.shape[2]
    nproj = beta.shape[2]
    streams = nb // LANES
    rows = gs.shape[2]
    parts = 2 if rows % 16 == 0 else 1
    rs = rows // parts
    halfn, zn = n // 2, n // 4
    share = nb // n
    core, xbit, mez, mej = me & 1, (me >> 1) & 1, me >> 2, me >> 1
    tile = block_of(nproj) if nproj % 256 else 256
    tiles = nproj // tile
    third = wr.shape[2]

    def beta_copy(t):
        at = pl.ds(pl.multiple_of(t * tile, tile), tile)
        return pltpu.make_async_copy(beta_hbm.at[0, :, :, at], beta.at[:, :, at], local_sems.at[t])

    small = [
        pltpu.make_async_copy(src, dst, local_sems.at[tiles + i])
        for i, (src, dst) in enumerate((
            (order_hbm, order), (wave_hbm.at[0], wave), (shift_hbm, shift), (phase_hbm, phase),
            (charge_hbm, charge.at[:, pl.ds(0, ppa), :]),
        ))
    ]
    barrier = pltpu.get_barrier_semaphore()
    greet = [{"pw": me ^ 1}, {"pw": me ^ 2}] + [{"pw": me ^ (d << 2)} for d in range(1, zn)]
    greet += [{"ka": ahead}] if paired else [{"ka": ahead}, {"ka": behind}]
    for where in greet:
        pl.semaphore_signal(barrier, inc=1, device_id=where, device_id_type=MESH)

    for copy in small[:2]:
        copy.start()
    depth = min(4, tiles)
    for t in range(depth):
        beta_copy(t).start()
    for copy in small[2:5]:
        copy.start()

    inverse_copies = [
        pltpu.make_async_copy(inv_v.at[b], inv_s.at[pl.ds(b * LANES, LANES)], local_sems.at[tiles + 5 + b])
        for b in range(inv_v.shape[0])
    ]
    def remote(src, dst, send, recv, where):
        return pltpu.make_async_remote_copy(
            src_ref=src, dst_ref=dst, send_sem=send, recv_sem=recv,
            device_id=where, device_id_type=MESH,
        )

    def invert():
        blocks = inv_v.shape[0]
        small[0].wait()
        slots = jnp.concatenate([order[r : r + 1, :] for r in range(nproj // LANES)], axis=1)
        upper, lower = jnp.right_shift(slots, 7), jnp.bitwise_and(slots, 127)
        place = lax.broadcasted_iota(jnp.int32, (1, nproj), 1)
        hot_u = lax.broadcasted_iota(jnp.int32, (blocks, nproj), 0) == upper
        hot_l = lax.broadcasted_iota(jnp.int32, (LANES, nproj), 0) == lower
        coarse = jnp.right_shift(place, 4).astype(jnp.float32)
        fine = jnp.bitwise_and(place, 15).astype(jnp.float32)
        left = jnp.concatenate([jnp.where(hot_u, coarse, 0.0), jnp.where(hot_u, fine, 0.0)], axis=0)
        found = dot(left.astype(jnp.bfloat16), jnp.where(hot_l, 1.0, 0.0).astype(jnp.bfloat16), (1, 1))
        found = (found[:blocks] * 16.0 + found[blocks:] + 0.5).astype(jnp.int32)
        inv_v[...] = jnp.clip(found, 0, nproj - 1)
        for copy in inverse_copies:
            copy.start()

    def transpose_waves():
        small[1].wait()
        for p in range(2):
            flat = wave[p].T
            for h in range(streams):
                mid = flat[h * LANES : (h + 1) * LANES]
                rhs[h, p, :LANES, :] = mid
                rhs[h, 1 - p, LANES:, :] = mid if p else -mid

    def multiply(hs, start, stop):
        def step(t, carry):
            if 0 in hs:
                beta_copy(t).wait()

                @pl.when(t + depth < tiles)
                def _():
                    beta_copy(t + depth).start()

            at = pl.ds(pl.multiple_of(t * tile, tile), tile)
            for h in hs:
                got = dot(rhs[h, 0], beta[0, :, at], (1, 0)) + dot(rhs[h, 1], beta[1, :, at], (1, 0))
                proj_t[h, :, at] = got
                peak = top[h]
                for b in range(tile // LANES):
                    peak = jnp.maximum(peak, jnp.abs(got[:, b * LANES : (b + 1) * LANES]))
                top[h] = peak
            return carry

        lax.fori_loop(start, stop, step, 0)

    def encode(h):
        peak = jnp.max(top[h], axis=1, keepdims=True)
        scale = jnp.maximum(peak, 1e-30) * (1.0 / TOP)
        inv_b[...] = jnp.broadcast_to(1.0 / scale, inv_b.shape)
        flat = jnp.broadcast_to(scale, inv_b.shape)
        sc0[h, 0:1, :] = flat[:LANES].T[0:1]
        sc0[h, 1:2, :] = flat[LANES:].T[0:1]

        def step(t, carry):
            at = pl.ds(pl.multiple_of(t * LANES, LANES), LANES)
            coded = pack(proj_t[h, :LANES, at], proj_t[h, LANES:, at], inv_b[:LANES], inv_b[LANES:])
            packed[at, :] = coded.T
            return carry

        lax.fori_loop(0, nproj // LANES, step, 0, unroll=3)

    def gather(dst, h, parity, sub):
        def one(j, carry):
            base = ((j << 1) | parity) * rows + sub * rs
            for g in range(rs // 8):
                slot = base + 8 * g
                taken = [packed[pl.ds(inv_s[slot + r], 1), :] for r in range(8)]
                dst[h, j, pl.ds(sub * rs + 8 * g, 8), :] = jnp.concatenate(taken, axis=0)
            return carry

        lax.fori_loop(0, halfn, one, 0)

    def span(sub):
        return pl.ds(sub * rs, rs)

    def core_copy(h, sub):
        return remote(
            gs.at[h, :, span(sub)], cr.at[h, :, span(sub)],
            core_sems.at[0, h, sub], core_sems.at[1, h, sub], {"pw": me ^ 1},
        )

    def core_scale_copy(h):
        return remote(sc0.at[h], sc0_r.at[h], core_scale_sems.at[0, h], core_scale_sems.at[1, h], {"pw": me ^ 1})

    def x_copies(h, sub):
        sems, where = x_sems, {"pw": me ^ 2}
        return [
            remote(xs.at[h, :, span(sub)], xr.at[h, :, span(sub)], sems.at[0, h, sub, 0], sems.at[1, h, sub, 0], where),
            remote(scx.at[h, sub], scx_r.at[h, sub], sems.at[0, h, sub, 1], sems.at[1, h, sub, 1], where),
        ]

    def z_copies(h, sub):
        made = []
        for d in range(1, zn):
            where = {"pw": me ^ (d << 2)}
            made.append(remote(
                zs.at[h, d - 1, span(sub)], zr.at[h, d - 1, span(sub)],
                z_sems.at[0, h, sub, d - 1, 0], z_sems.at[1, h, sub, d - 1, 0], where,
            ))
            made.append(remote(
                scz.at[h, sub], scz_r.at[h, sub, d - 1],
                z_sems.at[0, h, sub, d - 1, 1], z_sems.at[1, h, sub, d - 1, 1], where,
            ))
        return made

    def y_copies(h, sub):
        where = {"ka": behind}
        return [
            remote(ys.at[h, span(sub)], yr.at[h, span(sub)], y_sems.at[0, h, sub, 0], y_sems.at[1, h, sub, 0], where),
            remote(scy.at[h, sub], scy_r.at[h, sub], y_sems.at[0, h, sub, 1], y_sems.at[1, h, sub, 1], where),
        ]

    none = jnp.zeros((8, LANES), jnp.float32)

    def put_scale(ref, h, sub, tops):
        scales = [scale_of(t) for t in tops]
        ref[h, sub, 0:1, :] = scales[0]
        ref[h, sub, 1:2, :] = scales[1]
        return [1.0 / s for s in scales]

    def send_core(h, sub):
        gather(gs, h, 1 - core, sub)
        if sub == 0:
            core_scale_copy(h).start()
        core_copy(h, sub).start()

    def step_core(h, sub):
        if sub == 0:
            core_scale_copy(h).wait()
        core_copy(h, sub).wait()
        at = span(sub)
        own_r, own_i = sc0[h, 0:1, :], sc0[h, 1:2, :]
        sib_r, sib_i = sc0_r[h, 0:1, :], sc0_r[h, 1:2, :]

        def total(j):
            a, b = go[h, j, at, :], cr[h, j, at, :]
            return low(a) * own_r + low(b) * sib_r, high(a) * own_i + high(b) * sib_i

        def first(z, carry):
            tr, ti = carry
            real, imag = total((z << 1) | (1 - xbit))
            xf[z, 0], xf[z, 1] = real, imag
            return jnp.maximum(tr, fold(real)), jnp.maximum(ti, fold(imag))

        inv = put_scale(scx, h, sub, lax.fori_loop(0, zn, first, (none, none)))

        def second(z, carry):
            xs[h, z, at, :] = pack(xf[z, 0], xf[z, 1], *inv)
            return carry

        lax.fori_loop(0, zn, second, 0)
        for copy in x_copies(h, sub):
            copy.start()

        def keep(z, carry):
            real, imag = total((z << 1) | xbit)
            acc[h, z, 0, at, :] = real
            acc[h, z, 1, at, :] = imag
            return carry

        lax.fori_loop(0, zn, keep, 0)

    def step_x(h, sub):
        for copy in x_copies(h, sub):
            copy.wait()
        at = span(sub)
        s_r, s_i = scx_r[h, sub, 0:1, :], scx_r[h, sub, 1:2, :]

        def total(z):
            v = xr[h, z, at, :]
            real = acc[h, z, 0, at, :] + low(v) * s_r
            imag = acc[h, z, 1, at, :] + high(v) * s_i
            acc[h, z, 0, at, :] = real
            acc[h, z, 1, at, :] = imag
            return real, imag

        def first(d, carry):
            tr, ti = carry
            real, imag = total(mez ^ d)
            return jnp.maximum(tr, fold(real)), jnp.maximum(ti, fold(imag))

        inv = put_scale(scz, h, sub, lax.fori_loop(1, zn, first, (none, none)))

        def second(d, carry):
            z = mez ^ d
            zs[h, d - 1, at, :] = pack(acc[h, z, 0, at, :], acc[h, z, 1, at, :], *inv)
            return carry

        lax.fori_loop(1, zn, second, 0)
        for copy in z_copies(h, sub):
            copy.start()
        total(mez)

    def step_z(h, sub):
        for copy in z_copies(h, sub):
            copy.wait()
        at = span(sub)
        real, imag = acc[h, mez, 0, at, :], acc[h, mez, 1, at, :]
        for d in range(zn - 1):
            v = zr[h, d, at, :]
            real = real + low(v) * scz_r[h, sub, d, 0:1, :]
            imag = imag + high(v) * scz_r[h, sub, d, 1:2, :]
        cols = slice(h * LANES, (h + 1) * LANES)
        mine[0, at, cols] = real
        mine[1, at, cols] = imag
        inv = put_scale(scy, h, sub, (fold(real), fold(imag)))
        ys[h, at, :] = pack(real, imag, *inv)
        for copy in y_copies(h, sub):
            copy.start()

    def wave_copy(i, src):
        return remote(src, wr.at[i], wave_sems.at[0, i], wave_sems.at[1, i], {"ka": behind})

    def own_rows(i):
        return wave_hbm.at[0, :, pl.ds(i * third, third), :]

    def send_waves():
        if not paired:
            wave_copy(0, wave_hbm.at[0]).start()
            return

        @pl.when(k == 0)
        def _():
            wave_copy(0, own_rows(3)).start()

        @pl.when(k == 1)
        def _():
            for i in range(3):
                wave_copy(i, own_rows(i)).start()

    def spread_shift():
        small[2].wait()
        for b in range(pw_dev // LANES):
            line = shift[0:1, b * LANES : (b + 1) * LANES] - me * pw_dev
            spread[pl.ds(b * LANES, LANES), :] = jnp.broadcast_to(line, (LANES, LANES)).T

    def permute(dst, src, start, size, offset):
        block = min(block_of(size), 256)

        def step(b, carry):
            at = pl.ds(pl.multiple_of(start + b * block, block), block)
            to = pl.ds(pl.multiple_of(offset + b * block, block), block)
            want = spread[at, :]
            lane = lax.broadcasted_iota(jnp.int32, (block, LANES), 1)
            hot = jnp.concatenate(
                [jnp.where(want == lane + g * LANES, 1.0, 0.0) for g in range(pw_dev // LANES)], axis=1
            ).astype(jnp.bfloat16)
            for p in range(2):
                dst[p, to, :] = dot(hot, src(p), (1, 0)).astype(jnp.bfloat16)
            return carry

        lax.fori_loop(0, size // block, step, 0)

    def send_picked():
        @pl.when(k == 0)
        def _():
            permute(stage, lambda p: wave[p], 3 * third, third, 0)
            wave_copy(1, stage).start()

    def build_picked(i):
        @pl.when(k == 0)
        def _():
            permute(picked, lambda p: wave[p], i * third, third, i * third)

    def add(which, values, fresh):
        for c in range(2):
            if fresh:
                part[which, c] = values[c]
            else:
                part[which, c] += values[c]

    def piece(ref, i):
        return [ref[p, i * third : (i + 1) * third, :] for p in range(2)]

    def plane_first(i):
        @pl.when(k == 0)
        def _():
            wave_copy(i, own_rows(i)).wait_recv()
            got = [wr[i, 0], wr[i, 1]]
            add(0, cross(piece(wave, i), got), i == 0)
            add(1, cross(got, piece(picked, i)), i == 0)

    def plane_second(i):
        @pl.when(k == 1)
        def _():
            wave_copy(i, own_rows(i)).wait_recv()
            got = [wr[i, 0], wr[i, 1]]
            if i == 0:
                add(1, cross(got, piece(wave, 3)), True)
            else:
                add(0, cross(piece(wave, 3), got), True)

    def drain_waves():
        if not paired:
            wave_copy(0, wave_hbm.at[0]).wait_send()
            return

        @pl.when(k == 0)
        def _():
            wave_copy(0, own_rows(3)).wait_send()
            wave_copy(1, stage).wait_send()

        @pl.when(k == 1)
        def _():
            for i in range(3):
                wave_copy(i, own_rows(i)).wait_send()

    def plane_ring():
        wave_copy(0, wave_hbm.at[0]).wait_recv()

        @pl.when(last_k)
        def _():
            permute(picked, lambda p: wr[0, p], 0, pw_dev, 0)

        @pl.when(k != kn - 1)
        def _():
            picked[...] = wr[0]

        add(0, cross([wave[0], wave[1]], [picked[0], picked[1]]), True)

    def make_tables():
        small[3].wait()
        small[4].wait()
        atoms = phase.shape[1]
        own_atoms = rows // ppa
        row_i = lax.broadcasted_iota(jnp.int32, (rows, atoms), 0)
        lane = lax.broadcasted_iota(jnp.int32, (rows, atoms), 1)
        away = row_i - ppa * (lane - me * own_atoms)
        hit = (away >= 0) & (away < ppa)
        angle = jnp.where(last_k, phase[...], 0.0)
        cosine = jnp.sum(jnp.where(hit, jnp.cos(angle), 0.0), axis=1, keepdims=True)
        sine = jnp.sum(jnp.where(hit, jnp.sin(angle), 0.0), axis=1, keepdims=True)
        pad = charge.shape[1]
        flat = charge[...].reshape(ppa * pad, atoms)
        pick = jnp.where(hit, 1.0, 0.0)
        every = dot(pick, flat, (1, 1), HIGH)

        def iota(shape, axis):
            return lax.broadcasted_iota(jnp.int32, shape, axis).astype(jnp.float32)

        def div(x, by):
            return jnp.floor((x + 0.5) * (1.0 / by))

        shape = (rows, ppa * pad)
        r, c = iota(shape, 0), iota(shape, 1)
        own_p = r - ppa * div(r, ppa)
        col_p = div(c, pad)
        kept = jnp.where((own_p == col_p) & (c - pad * col_p < ppa), every, 0.0)
        shape = (ppa * pad, rows)
        c, j = iota(shape, 0), iota(shape, 1)
        widen = jnp.where(c - pad * div(c, pad) == j - ppa * div(j, ppa), 1.0, 0.0)
        full = dot(kept, widen, (1, 0), HIGH) + dot(widen, kept, (0, 1), HIGH)
        shape = (rows, rows)
        same = div(iota(shape, 0), ppa) == div(iota(shape, 1), ppa)
        sym[...] = jnp.where(same, 0.5 * full, 0.0)
        return cosine, sine

    def m_copies(w):
        where = {"pw": me ^ 1}
        return [
            remote(ms.at[w], mr.at[w], m_sems.at[0, w, 0], m_sems.at[1, w, 0], where),
            remote(scm.at[w], scm_r.at[w], m_sems.at[0, w, 1], m_sems.at[1, w, 1], where),
        ]

    def d_copies(w):
        made = []
        for d in range(1 - w, halfn):
            where = {"pw": me ^ (d << 1)}
            if w:
                where["ka"] = ahead
            made.append(remote(
                ds.at[w, d], dr.at[w, d], d_sems.at[0, w, d, 0], d_sems.at[1, w, d, 0], where,
            ))
            made.append(remote(
                scd.at[w], scd_r.at[w, d], d_sems.at[0, w, d, 1], d_sems.at[1, w, d, 1], where,
            ))
        return made

    wide = jnp.zeros((8, nb), jnp.float32)

    def block_at(j, parity):
        return pl.ds(pl.multiple_of(((j << 1) | parity) * share, share), share)

    def margin_scale(ref, w, tops):
        scales = [scale_of(t) for t in tops]
        ref[w, 0:1, :] = scales[0]
        ref[w, 1:2, :] = scales[1]
        return [1.0 / s for s in scales]

    def send_margin(w):
        def first(j, carry):
            at = block_at(j, 1 - core)
            return jnp.maximum(carry[0], fold(part[w, 0, at, :])), jnp.maximum(carry[1], fold(part[w, 1, at, :]))

        inv = margin_scale(scm, w, lax.fori_loop(0, halfn, first, (wide, wide)))

        def second(j, carry):
            at = block_at(j, 1 - core)
            ms[w, j] = pack(part[w, 0, at, :], part[w, 1, at, :], *inv)
            return carry

        lax.fori_loop(0, halfn, second, 0)
        for copy in m_copies(w):
            copy.start()

    def step_margin(w):
        for copy in m_copies(w):
            copy.wait()
        s_r, s_i = scm_r[w, 0:1, :], scm_r[w, 1:2, :]

        def first(d, carry):
            j = mej ^ d
            at = block_at(j, core)
            v = mr[w, j]
            real = part[w, 0, at, :] + low(v) * s_r
            imag = part[w, 1, at, :] + high(v) * s_i
            macc[w, d, 0], macc[w, d, 1] = real, imag
            return jnp.maximum(carry[0], fold(real)), jnp.maximum(carry[1], fold(imag))

        inv = margin_scale(scd, w, lax.fori_loop(0, halfn, first, (wide, wide)))

        def second(d, carry):
            ds[w, d] = pack(macc[w, d, 0], macc[w, d, 1], *inv)
            return carry

        lax.fori_loop(1 - w, halfn, second, 0)
        for copy in d_copies(w):
            copy.start()

    def finish_margin(w, real, imag):
        for copy in d_copies(w):
            copy.wait()
        for d in range(1 - w, halfn):
            v = dr[w, d]
            real = real + low(v) * scd_r[w, d, 0:1, :]
            imag = imag + high(v) * scd_r[w, d, 1:2, :]
        return real, imag

    last = streams - 1
    early = tiles // 3
    invert()
    transpose_waves()
    top[...] = jnp.zeros_like(top)
    multiply(range(streams), 0, early)
    pl.semaphore_wait(barrier, len(greet))
    send_waves()
    multiply((0,), early, tiles)
    for h in range(streams):
        if h > 0:
            multiply((h,), early, tiles)
        encode(h)
        if h == 0:
            for copy in inverse_copies:
                copy.wait()
        for sub in range(parts):
            send_core(h, sub)
        for sub in range(parts):
            gather(go, h, core, sub)
            step_core(h, sub)
            if h > 0:
                step_x(h - 1, sub)
    spread_shift()
    if paired:
        send_picked()
        build_picked(0)
    if paired:
        plane_first(0)
        plane_second(0)
    step_x(last, 0)
    if paired:
        build_picked(1)
        plane_first(1)
    for sub in range(1, parts):
        step_x(last, sub)
    for h in range(last):
        for sub in range(parts):
            step_z(h, sub)
    if paired:
        build_picked(2)
    cosine, sine = make_tables()
    for sub in range(parts):
        step_z(last, sub)
    for h in range(last):
        for sub in range(parts):
            for copy in y_copies(h, sub):
                copy.wait()
    if paired:
        plane_first(2)
        send_margin(1)
        plane_second(1)
        step_margin(1)
    else:
        plane_ring()
    for sub in range(parts):
        for copy in y_copies(last, sub):
            copy.wait()

    def next_part(take, c):
        lines = []
        for sub in range(parts):
            pieces = [take(yr[h, span(sub), :]) * scy_r[h, sub, c : c + 1, :] for h in range(streams)]
            lines.append(jnp.concatenate(pieces, axis=1))
        return jnp.concatenate(lines, axis=0)

    nr, ni = next_part(low, 0), next_part(high, 1)
    turned = jnp.concatenate([nr * cosine + ni * sine, ni * cosine - nr * sine], axis=1)
    weighted = dot(sym[...], turned, (1, 0), HIGH)
    by_real = contract(mine[0], weighted, HIGH)
    by_imag = contract(mine[1], weighted, HIGH)
    part[0, 0] += by_real[:, :nb] + by_imag[:, nb:]
    part[0, 1] += by_real[:, nb:] - by_imag[:, :nb]
    send_margin(0)
    step_margin(0)
    real, imag = macc[0, 0, 0], macc[0, 0, 1]
    if paired:
        real, imag = finish_margin(1, real, imag)
    real, imag = finish_margin(0, real, imag)
    drain_waves()
    out[:, 0, :] = real
    out[:, 1, :] = imag


def fused(n, kn, order, shift, phase, charges, waves, projectors):
    pw_dev, nb = waves.shape[2], waves.shape[3]
    nproj = projectors.shape[3]
    atoms = phase.shape[1]
    ppa = charges.shape[0]
    rows, share = nproj // n, nb // n
    h = nb // LANES
    parts = 2 if rows % 16 == 0 else 1
    zn, half = n // 4, n // 2
    pad = -(-ppa // 8) * 8
    blocks = -(-nproj // (8 * LANES)) * 8
    paired = kn == 2
    slots, third = (3, pw_dev // 4) if paired else (1, pw_dev)
    kinds = 2 if paired else 1
    anywhere = pl.BlockSpec(memory_space=pl.ANY)
    f32, i32, bf16 = jnp.float32, jnp.int32, jnp.bfloat16
    tile = block_of(nproj) if nproj % 256 else 256
    scratch = [
        ((nproj // LANES, LANES), i32), ((1, pw_dev), i32), ((1, atoms), f32), ((ppa, pad, atoms), f32),
        ((blocks, LANES), i32), "smem", ((pw_dev, LANES), i32), ((rows, rows), f32),
        ((2, pw_dev, nb), bf16), ((2, pw_dev, nproj), bf16), ((h, 2, 2 * LANES, pw_dev), bf16),
        ((h, 2 * LANES, nproj), f32), ((h, 2 * LANES, LANES), f32), ((2 * LANES, LANES), f32), ((nproj, LANES), i32),
        ((h, half, rows, LANES), i32), ((h, half, rows, LANES), i32), ((h, half, rows, LANES), i32),
        ((h, 2, LANES), f32), ((h, 2, LANES), f32),
        ((zn, 2, rows // parts, LANES), f32), ((h, zn, rows, LANES), i32), ((h, zn, rows, LANES), i32),
        ((h, parts, 2, LANES), f32), ((h, parts, 2, LANES), f32), ((h, zn, 2, rows, LANES), f32),
        ((h, zn - 1, rows, LANES), i32), ((h, zn - 1, rows, LANES), i32),
        ((h, parts, 2, LANES), f32), ((h, parts, zn - 1, 2, LANES), f32), ((2, rows, nb), f32),
        ((h, rows, LANES), i32), ((h, rows, LANES), i32), ((h, parts, 2, LANES), f32), ((h, parts, 2, LANES), f32),
        ((slots, 2, third, nb), bf16), ((2, slots * third, nb), bf16), ((2, third, nb), bf16),
        ((kinds, 2, nb, nb), f32), ((kinds, half, share, nb), i32), ((kinds, half, share, nb), i32),
        ((kinds, 2, nb), f32), ((kinds, 2, nb), f32), ((kinds, half, 2, share, nb), f32),
        ((kinds, half, share, nb), i32), ((kinds, half, share, nb), i32),
        ((kinds, 2, nb), f32), ((kinds, half, 2, nb), f32),
    ]
    made = [pltpu.SMEM((blocks * LANES,), i32) if s == "smem" else pltpu.VMEM(*s) for s in scratch]
    sems = [
        (nproj // tile + 5 + blocks,), (2, h, parts), (2, h), (2, h, parts, 2), (2, h, parts, zn - 1, 2),
        (2, h, parts, 2), (2, slots), (2, kinds, 2), (2, kinds, half, 2),
    ]
    return pl.pallas_call(
        functools.partial(fused_kernel, n, kn, ppa),
        out_shape=jax.ShapeDtypeStruct((share, 2, nb), f32),
        in_specs=[anywhere] * 6,
        out_specs=pl.BlockSpec(memory_space=pltpu.VMEM),
        scratch_shapes=made + [pltpu.SemaphoreType.DMA(s) for s in sems],
        compiler_params=pltpu.CompilerParams(
            collective_id=0, has_side_effects=True, vmem_limit_bytes=62 * 2**20
        ),
    )(order, shift, phase, charges, waves, projectors)


def local(waves, projectors, projector_order, shift_map, charges, atom_phase):
    n = lax.axis_size("pw")
    kn = lax.axis_size("ka")
    summed = fused(
        n, kn, projector_order.reshape(-1, LANES), shift_map[None, :], atom_phase[None, :],
        jnp.transpose(charges, (1, 2, 0)), waves, projectors,
    )
    return summed[None]


def solution(mesh):
    placed = (P("ka", None, "pw", None), P("ka", None, "pw", None), P(), P("pw"), P(), P())
    return jax.shard_map(
        local, mesh=mesh, in_specs=placed, out_specs=P("ka", "pw", None, None), check_vma=False
    )
```

```python
import functools
import math

import jax
import jax.numpy as jnp
from jax import lax
from jax.experimental import pallas as pl
from jax.experimental.pallas import tpu as pltpu
from jax.sharding import PartitionSpec as P

MESH = pl.DeviceIdType.MESH
LANES = 128
TOP = 32767.0
HIGH = lax.Precision.HIGHEST


def dot(left, right, dims, precision=None):
    return lax.dot_general(
        left, right, (((dims[0],), (dims[1],)), ((), ())),
        precision=precision, preferred_element_type=jnp.float32,
    )


def contract(left, right, precision=None):
    return dot(left, right, (0, 0), precision)


def cross(left, right):
    real = contract(left[0], right[0]) + contract(left[1], right[1])
    imag = contract(left[0], right[1]) - contract(left[1], right[0])
    return real, imag


def low(v):
    return jnp.right_shift(jnp.left_shift(v, 16), 16).astype(jnp.float32)


def high(v):
    return jnp.right_shift(v, 16).astype(jnp.float32)


def code(x, inv):
    return jnp.floor(x * inv + 0.5).astype(jnp.int32)


def pack(real, imag, inv_real, inv_imag):
    return jnp.bitwise_or(
        jnp.left_shift(code(imag, inv_imag), 16),
        jnp.bitwise_and(code(real, inv_real), 0xFFFF),
    )


def fold(x):
    return jnp.max(jnp.abs(x).reshape(x.shape[0] // 8, 8, x.shape[1]), axis=0)


def scale_of(top):
    return jnp.maximum(jnp.max(top, axis=0, keepdims=True), 1e-30) * (1.0 / TOP)


def block_of(size):
    for block in (512, 256, 128):
        if size % block == 0:
            return block
    return size


def pieces_of(rows, ppa):
    return 2 if rows % 16 == 0 and (rows // 2) % ppa == 0 else 1


def fused_kernel(
    n, kn, ppa, order_hbm, shift_hbm, phase_hbm, charge_hbm, wave_hbm, beta_hbm, out,
    order, shift, phase, charge, inv_v, inv_s, spread, sym, wave, beta, rhs, proj_t, top, inv_b, packed,
    gs, go, cr, sc0, sc0_r, xf, xs, xr, scx, scx_r, acc, zs, zr, scz, scz_r, mine, ys, yr, scy, scy_r,
    wr, picked, stage, part, ms, mr, scm, scm_r, macc, ds, dr, scd, scd_r,
    local_sems, core_sems, core_scale_sems, x_sems, z_sems, y_sems, wave_sems, m_sems, d_sems,
):
    me = lax.axis_index("pw")
    k = lax.axis_index("ka")
    ahead, behind = lax.rem(k + 1, kn), lax.rem(k + kn - 1, kn)
    last_k = k == kn - 1
    paired = kn == 2
    pw_dev, nb = wave.shape[1], wave.shape[2]
    nproj = beta.shape[2]
    streams = nb // LANES
    rows = gs.shape[2]
    parts = pieces_of(rows, ppa)
    rs = rows // parts
    halfn, zn = n // 2, n // 4
    share = nb // n
    core, xbit, mez, mej = me & 1, (me >> 1) & 1, me >> 2, me >> 1
    tile = block_of(nproj) if nproj % 256 else 256
    tiles = nproj // tile
    unit = pw_dev // 16
    cuts = ((0, 4, 8, 11), (0, 5, 10))
    few = 11 * unit

    def beta_copy(t):
        at = pl.ds(pl.multiple_of(t * tile, tile), tile)
        return pltpu.make_async_copy(beta_hbm.at[0, :, :, at], beta.at[:, :, at], local_sems.at[t])

    small = [
        pltpu.make_async_copy(src, dst, local_sems.at[tiles + i])
        for i, (src, dst) in enumerate((
            (order_hbm, order), (wave_hbm.at[0], wave), (shift_hbm, shift), (phase_hbm, phase),
            (charge_hbm, charge.at[:, pl.ds(0, ppa), :]),
        ))
    ]
    barrier = pltpu.get_barrier_semaphore()
    greet = [{"pw": me ^ 1}, {"pw": me ^ 2}] + [{"pw": me ^ (d << 2)} for d in range(1, zn)]
    greet += [{"ka": ahead}] if paired else [{"ka": ahead}, {"ka": behind}]
    for where in greet:
        pl.semaphore_signal(barrier, inc=1, device_id=where, device_id_type=MESH)

    for copy in small[:2]:
        copy.start()
    depth = min(4, tiles)
    for t in range(depth):
        beta_copy(t).start()
    for copy in small[2:5]:
        copy.start()

    inverse_copies = [
        pltpu.make_async_copy(inv_v.at[b], inv_s.at[pl.ds(b * LANES, LANES)], local_sems.at[tiles + 5 + b])
        for b in range(inv_v.shape[0])
    ]
    def remote(src, dst, send, recv, where):
        return pltpu.make_async_remote_copy(
            src_ref=src, dst_ref=dst, send_sem=send, recv_sem=recv,
            device_id=where, device_id_type=MESH,
        )

    def invert():
        blocks = inv_v.shape[0]
        small[0].wait()
        slots = jnp.concatenate([order[r : r + 1, :] for r in range(nproj // LANES)], axis=1)
        upper, lower = jnp.right_shift(slots, 7), jnp.bitwise_and(slots, 127)
        place = lax.broadcasted_iota(jnp.int32, (1, nproj), 1)
        hot_u = lax.broadcasted_iota(jnp.int32, (blocks, nproj), 0) == upper
        hot_l = lax.broadcasted_iota(jnp.int32, (LANES, nproj), 0) == lower
        coarse = jnp.right_shift(place, 4).astype(jnp.float32)
        fine = jnp.bitwise_and(place, 15).astype(jnp.float32)
        left = jnp.concatenate([jnp.where(hot_u, coarse, 0.0), jnp.where(hot_u, fine, 0.0)], axis=0)
        found = dot(left.astype(jnp.bfloat16), jnp.where(hot_l, 1.0, 0.0).astype(jnp.bfloat16), (1, 1))
        found = (found[:blocks] * 16.0 + found[blocks:] + 0.5).astype(jnp.int32)
        inv_v[...] = jnp.clip(found, 0, nproj - 1)
        for copy in inverse_copies:
            copy.start()

    def transpose_waves():
        small[1].wait()
        for p in range(2):
            flat = wave[p].T
            for h in range(streams):
                mid = flat[h * LANES : (h + 1) * LANES]
                rhs[h, p, :LANES, :] = mid
                rhs[h, 1 - p, LANES:, :] = mid if p else -mid

    def multiply(hs, start, stop):
        def step(t, carry):
            if 0 in hs:
                beta_copy(t).wait()

                @pl.when(t + depth < tiles)
                def _():
                    beta_copy(t + depth).start()

            at = pl.ds(pl.multiple_of(t * tile, tile), tile)
            for h in hs:
                got = dot(rhs[h, 0], beta[0, :, at], (1, 0)) + dot(rhs[h, 1], beta[1, :, at], (1, 0))
                proj_t[h, :, at] = got
                peak = top[h]
                for b in range(tile // LANES):
                    peak = jnp.maximum(peak, jnp.abs(got[:, b * LANES : (b + 1) * LANES]))
                top[h] = peak
            return carry

        lax.fori_loop(start, stop, step, 0)

    def encode(h):
        peak = jnp.max(top[h], axis=1, keepdims=True)
        scale = jnp.maximum(peak, 1e-30) * (1.0 / TOP)
        inv_b[...] = jnp.broadcast_to(1.0 / scale, inv_b.shape)
        flat = jnp.broadcast_to(scale, inv_b.shape)
        sc0[h, 0:1, :] = flat[:LANES].T[0:1]
        sc0[h, 1:2, :] = flat[LANES:].T[0:1]

        def step(t, carry):
            at = pl.ds(pl.multiple_of(t * LANES, LANES), LANES)
            coded = pack(proj_t[h, :LANES, at], proj_t[h, LANES:, at], inv_b[:LANES], inv_b[LANES:])
            packed[at, :] = coded.T
            return carry

        lax.fori_loop(0, nproj // LANES, step, 0, unroll=3)

    def gather(dst, h, parity, sub):
        def one(j, carry):
            base = ((j << 1) | parity) * rows + sub * rs
            for g in range(rs // 8):
                slot = base + 8 * g
                taken = [packed[pl.ds(inv_s[slot + r], 1), :] for r in range(8)]
                dst[h, j, pl.ds(sub * rs + 8 * g, 8), :] = jnp.concatenate(taken, axis=0)
            return carry

        lax.fori_loop(0, halfn, one, 0)

    def span(sub):
        return pl.ds(sub * rs, rs)

    def core_copy(h, sub):
        return remote(
            gs.at[h, :, span(sub)], cr.at[h, :, span(sub)],
            core_sems.at[0, h, sub], core_sems.at[1, h, sub], {"pw": me ^ 1},
        )

    def core_scale_copy(h):
        return remote(sc0.at[h], sc0_r.at[h], core_scale_sems.at[0, h], core_scale_sems.at[1, h], {"pw": me ^ 1})

    def x_copies(h, sub):
        sems, where = x_sems, {"pw": me ^ 2}
        return [
            remote(xs.at[h, :, span(sub)], xr.at[h, :, span(sub)], sems.at[0, h, sub, 0], sems.at[1, h, sub, 0], where),
            remote(scx.at[h, sub], scx_r.at[h, sub], sems.at[0, h, sub, 1], sems.at[1, h, sub, 1], where),
        ]

    def z_copies(h, sub):
        made = []
        for d in range(1, zn):
            where = {"pw": me ^ (d << 2)}
            made.append(remote(
                zs.at[h, d - 1, span(sub)], zr.at[h, d - 1, span(sub)],
                z_sems.at[0, h, sub, d - 1, 0], z_sems.at[1, h, sub, d - 1, 0], where,
            ))
            made.append(remote(
                scz.at[h, sub], scz_r.at[h, sub, d - 1],
                z_sems.at[0, h, sub, d - 1, 1], z_sems.at[1, h, sub, d - 1, 1], where,
            ))
        return made

    def y_copies(h, sub):
        where = {"ka": behind}
        return [
            remote(ys.at[h, span(sub)], yr.at[h, span(sub)], y_sems.at[0, h, sub, 0], y_sems.at[1, h, sub, 0], where),
            remote(scy.at[h, sub], scy_r.at[h, sub], y_sems.at[0, h, sub, 1], y_sems.at[1, h, sub, 1], where),
        ]

    none = jnp.zeros((8, LANES), jnp.float32)

    def put_scale(ref, h, sub, tops):
        scales = [scale_of(t) for t in tops]
        ref[h, sub, 0:1, :] = scales[0]
        ref[h, sub, 1:2, :] = scales[1]
        return [1.0 / s for s in scales]

    def send_core(h, sub):
        gather(gs, h, 1 - core, sub)
        if sub == 0:
            core_scale_copy(h).start()
        core_copy(h, sub).start()

    def step_core(h, sub):
        if sub == 0:
            core_scale_copy(h).wait()
        core_copy(h, sub).wait()
        at = span(sub)
        own_r, own_i = sc0[h, 0:1, :], sc0[h, 1:2, :]
        sib_r, sib_i = sc0_r[h, 0:1, :], sc0_r[h, 1:2, :]

        def total(j):
            a, b = go[h, j, at, :], cr[h, j, at, :]
            return low(a) * own_r + low(b) * sib_r, high(a) * own_i + high(b) * sib_i

        def first(z, carry):
            tr, ti = carry
            real, imag = total((z << 1) | (1 - xbit))
            xf[z, 0], xf[z, 1] = real, imag
            return jnp.maximum(tr, fold(real)), jnp.maximum(ti, fold(imag))

        inv = put_scale(scx, h, sub, lax.fori_loop(0, zn, first, (none, none)))

        def second(z, carry):
            xs[h, z, at, :] = pack(xf[z, 0], xf[z, 1], *inv)
            return carry

        lax.fori_loop(0, zn, second, 0)
        for copy in x_copies(h, sub):
            copy.start()

        def keep(z, carry):
            real, imag = total((z << 1) | xbit)
            acc[h, z, 0, at, :] = real
            acc[h, z, 1, at, :] = imag
            return carry

        lax.fori_loop(0, zn, keep, 0)

    def step_x(h, sub):
        for copy in x_copies(h, sub):
            copy.wait()
        at = span(sub)
        s_r, s_i = scx_r[h, sub, 0:1, :], scx_r[h, sub, 1:2, :]

        def total(z):
            v = xr[h, z, at, :]
            real = acc[h, z, 0, at, :] + low(v) * s_r
            imag = acc[h, z, 1, at, :] + high(v) * s_i
            acc[h, z, 0, at, :] = real
            acc[h, z, 1, at, :] = imag
            return real, imag

        def first(d, carry):
            tr, ti = carry
            real, imag = total(mez ^ d)
            return jnp.maximum(tr, fold(real)), jnp.maximum(ti, fold(imag))

        inv = put_scale(scz, h, sub, lax.fori_loop(1, zn, first, (none, none)))

        def second(d, carry):
            z = mez ^ d
            zs[h, d - 1, at, :] = pack(acc[h, z, 0, at, :], acc[h, z, 1, at, :], *inv)
            return carry

        lax.fori_loop(1, zn, second, 0)
        for copy in z_copies(h, sub):
            copy.start()
        total(mez)

    def step_z(h, sub):
        for copy in z_copies(h, sub):
            copy.wait()
        at = span(sub)
        real, imag = acc[h, mez, 0, at, :], acc[h, mez, 1, at, :]
        for d in range(zn - 1):
            v = zr[h, d, at, :]
            real = real + low(v) * scz_r[h, sub, d, 0:1, :]
            imag = imag + high(v) * scz_r[h, sub, d, 1:2, :]
        cols = slice(h * LANES, (h + 1) * LANES)
        mine[0, at, cols] = real
        mine[1, at, cols] = imag
        inv = put_scale(scy, h, sub, (fold(real), fold(imag)))
        ys[h, at, :] = pack(real, imag, *inv)
        for copy in y_copies(h, sub):
            copy.start()

    def wave_copy(i, src, at):
        return remote(src, wr.at[:, at, :], wave_sems.at[0, i], wave_sems.at[1, i], {"ka": behind})

    def landing(side, i):
        low_end, high_end = cuts[side][i : i + 2]
        return pl.ds(low_end * unit, (high_end - low_end) * unit)

    def sent(side, i):
        if side == 1:
            return wave_copy(i, wave.at[:, landing(0, i), :], landing(0, i))
        src = stage if i else wave.at[:, pl.ds(few, pw_dev - few), :]
        return wave_copy(i, src, landing(1, i))

    def whole_wave():
        return wave_copy(0, wave, pl.ds(0, pw_dev))

    def send_waves():
        if not paired:
            whole_wave().start()
            return

        @pl.when(k == 0)
        def _():
            sent(0, 0).start()

        @pl.when(k == 1)
        def _():
            for i in range(3):
                sent(1, i).start()

    def spread_shift():
        small[2].wait()
        for b in range(pw_dev // LANES):
            line = shift[0:1, b * LANES : (b + 1) * LANES] - me * pw_dev
            spread[pl.ds(b * LANES, LANES), :] = jnp.broadcast_to(line, (LANES, LANES)).T

    def permute(dst, src, start, size, offset):
        block = next((b for b in (256, 192, 320, 128) if size % b == 0), size)

        def step(b, carry):
            at = pl.ds(pl.multiple_of(start + b * block, math.gcd(start, block)), block)
            to = pl.ds(pl.multiple_of(offset + b * block, math.gcd(offset, block)), block)
            want = spread[at, :]
            lane = lax.broadcasted_iota(jnp.int32, (block, LANES), 1)
            hot = jnp.concatenate(
                [jnp.where(want == lane + g * LANES, 1.0, 0.0) for g in range(pw_dev // LANES)], axis=1
            ).astype(jnp.bfloat16)
            for p in range(2):
                dst[p, to, :] = dot(hot, src(p), (1, 0)).astype(jnp.bfloat16)
            return carry

        lax.fori_loop(0, size // block, step, 0)

    def send_picked():
        @pl.when(k == 0)
        def _():
            permute(stage, lambda p: wave[p], few, pw_dev - few, 0)
            sent(0, 1).start()

    def build_picked(i):
        @pl.when(k == 0)
        def _():
            start, stop = cuts[0][i] * unit, cuts[0][i + 1] * unit
            permute(picked, lambda p: wave[p], start, stop - start, start)

    def add(which, values, fresh):
        for c in range(2):
            if fresh:
                part[which, c] = values[c]
            else:
                part[which, c] += values[c]

    def piece(ref, start, stop):
        return [ref[p, start:stop, :] for p in range(2)]

    def plane_first(i):
        @pl.when(k == 0)
        def _():
            sent(1, i).wait_recv()
            ends = cuts[0][i] * unit, cuts[0][i + 1] * unit
            got = piece(wr, *ends)
            add(0, cross(piece(wave, *ends), got), i == 0)
            add(1, cross(got, piece(picked, *ends)), i == 0)

    def plane_second(i):
        @pl.when(k == 1)
        def _():
            sent(0, i).wait_recv()
            got = piece(wr, cuts[1][i] * unit, cuts[1][i + 1] * unit)
            rest = piece(wave, few, pw_dev)
            if i == 0:
                add(1, cross(got, rest), True)
            else:
                add(0, cross(rest, got), True)

    def drain_waves():
        if not paired:
            whole_wave().wait_send()
            return

        @pl.when(k == 0)
        def _():
            for i in range(2):
                sent(0, i).wait_send()

        @pl.when(k == 1)
        def _():
            for i in range(3):
                sent(1, i).wait_send()

    def plane_ring():
        whole_wave().wait_recv()

        @pl.when(last_k)
        def _():
            permute(picked, lambda p: wr[p], 0, pw_dev, 0)

        @pl.when(k != kn - 1)
        def _():
            picked[...] = wr[...]

        add(0, cross([wave[0], wave[1]], [picked[0], picked[1]]), True)

    def make_tables():
        small[3].wait()
        small[4].wait()
        atoms = phase.shape[1]
        own_atoms = rows // ppa
        row_i = lax.broadcasted_iota(jnp.int32, (rows, atoms), 0)
        lane = lax.broadcasted_iota(jnp.int32, (rows, atoms), 1)
        away = row_i - ppa * (lane - me * own_atoms)
        hit = (away >= 0) & (away < ppa)
        angle = jnp.where(last_k, phase[...], 0.0)
        cosine = jnp.sum(jnp.where(hit, jnp.cos(angle), 0.0), axis=1, keepdims=True)
        sine = jnp.sum(jnp.where(hit, jnp.sin(angle), 0.0), axis=1, keepdims=True)
        pad = charge.shape[1]
        flat = charge[...].reshape(ppa * pad, atoms)
        pick = jnp.where(hit, 1.0, 0.0)
        every = dot(pick, flat, (1, 1), HIGH)

        def iota(shape, axis):
            return lax.broadcasted_iota(jnp.int32, shape, axis).astype(jnp.float32)

        def div(x, by):
            return jnp.floor((x + 0.5) * (1.0 / by))

        shape = (rows, ppa * pad)
        r, c = iota(shape, 0), iota(shape, 1)
        own_p = r - ppa * div(r, ppa)
        col_p = div(c, pad)
        kept = jnp.where((own_p == col_p) & (c - pad * col_p < ppa), every, 0.0)
        shape = (ppa * pad, rows)
        c, j = iota(shape, 0), iota(shape, 1)
        widen = jnp.where(c - pad * div(c, pad) == j - ppa * div(j, ppa), 1.0, 0.0)
        full = dot(kept, widen, (1, 0), HIGH) + dot(widen, kept, (0, 1), HIGH)
        shape = (rows, rows)
        same = div(iota(shape, 0), ppa) == div(iota(shape, 1), ppa)
        sym[...] = jnp.where(same, 0.5 * full, 0.0)
        return cosine, sine

    def m_copies(w, h):
        where = {"pw": me ^ 1}
        return [
            remote(ms.at[w, h], mr.at[w, h], m_sems.at[0, w, h, 0], m_sems.at[1, w, h, 0], where),
            remote(scm.at[w, h], scm_r.at[w, h], m_sems.at[0, w, h, 1], m_sems.at[1, w, h, 1], where),
        ]

    def d_copies(w, h):
        made = []
        for d in range(1 - w, halfn):
            where = {"pw": me ^ (d << 1)}
            if w:
                where["ka"] = ahead
            made.append(remote(
                ds.at[w, h, d], dr.at[w, h, d], d_sems.at[0, w, h, d, 0], d_sems.at[1, w, h, d, 0], where,
            ))
            made.append(remote(
                scd.at[w, h], scd_r.at[w, h, d], d_sems.at[0, w, h, d, 1], d_sems.at[1, w, h, d, 1], where,
            ))
        return made

    def block_at(j, parity):
        return pl.ds(pl.multiple_of(((j << 1) | parity) * share, share), share)

    def columns(h):
        return slice(h * LANES, (h + 1) * LANES)

    def send_margin(w, h):
        cols = columns(h)

        def first(j, carry):
            at = block_at(j, 1 - core)
            return (
                jnp.maximum(carry[0], fold(part[w, 0, at, cols])),
                jnp.maximum(carry[1], fold(part[w, 1, at, cols])),
            )

        inv = put_scale(scm, w, h, lax.fori_loop(0, halfn, first, (none, none)))

        def second(j, carry):
            at = block_at(j, 1 - core)
            ms[w, h, j] = pack(part[w, 0, at, cols], part[w, 1, at, cols], *inv)
            return carry

        lax.fori_loop(0, halfn, second, 0)
        for copy in m_copies(w, h):
            copy.start()

    def step_margin(w, h):
        for copy in m_copies(w, h):
            copy.wait()
        cols = columns(h)
        s_r, s_i = scm_r[w, h, 0:1, :], scm_r[w, h, 1:2, :]

        def first(d, carry):
            j = mej ^ d
            at = block_at(j, core)
            v = mr[w, h, j]
            real = part[w, 0, at, cols] + low(v) * s_r
            imag = part[w, 1, at, cols] + high(v) * s_i
            macc[w, h, d, 0], macc[w, h, d, 1] = real, imag
            return jnp.maximum(carry[0], fold(real)), jnp.maximum(carry[1], fold(imag))

        inv = put_scale(scd, w, h, lax.fori_loop(0, halfn, first, (none, none)))

        def second(d, carry):
            ds[w, h, d] = pack(macc[w, h, d, 0], macc[w, h, d, 1], *inv)
            return carry

        lax.fori_loop(1 - w, halfn, second, 0)
        for copy in d_copies(w, h):
            copy.start()

    def finish_margin(w, h, real, imag):
        for copy in d_copies(w, h):
            copy.wait()
        for d in range(1 - w, halfn):
            v = dr[w, h, d]
            real = real + low(v) * scd_r[w, h, d, 0:1, :]
            imag = imag + high(v) * scd_r[w, h, d, 1:2, :]
        return real, imag

    def augment(h, sub, cosine, sine):
        for copy in y_copies(h, sub):
            copy.wait()
        at = slice(sub * rs, (sub + 1) * rs)
        v = yr[h, at, :]
        nr, ni = low(v) * scy_r[h, sub, 0:1, :], high(v) * scy_r[h, sub, 1:2, :]
        c, s = cosine[at], sine[at]
        turned = jnp.concatenate([nr * c + ni * s, ni * c - nr * s], axis=1)
        weighted = dot(sym[at, at], turned, (1, 0), HIGH)
        by_real = contract(mine[0, at, :], weighted, HIGH)
        by_imag = contract(mine[1, at, :], weighted, HIGH)
        cols = columns(h)
        part[0, 0, :, cols] += by_real[:, :LANES] + by_imag[:, LANES:]
        part[0, 1, :, cols] += by_real[:, LANES:] - by_imag[:, :LANES]

    last = streams - 1
    early = tiles // 3
    invert()
    transpose_waves()
    top[...] = jnp.zeros_like(top)
    multiply(range(streams), 0, early)
    pl.semaphore_wait(barrier, len(greet))
    send_waves()
    multiply((0,), early, tiles)
    for h in range(streams):
        if h > 0:
            multiply((h,), early, tiles)
        encode(h)
        if h == 0:
            for copy in inverse_copies:
                copy.wait()
        for sub in range(parts):
            send_core(h, sub)
        for sub in range(parts):
            gather(go, h, core, sub)
            step_core(h, sub)
            if h > 0:
                step_x(h - 1, sub)
    spread_shift()
    if paired:
        send_picked()
        build_picked(0)
    if paired:
        plane_first(0)
        plane_second(0)
    step_x(last, 0)
    if paired:
        build_picked(1)
        plane_first(1)
    for sub in range(1, parts):
        step_x(last, sub)
    for h in range(last):
        for sub in range(parts):
            step_z(h, sub)
    if paired:
        build_picked(2)
    cosine, sine = make_tables()
    for sub in range(parts):
        step_z(last, sub)
    if paired:
        plane_first(2)
        plane_second(1)
    else:
        plane_ring()
    for h in range(last):
        for sub in range(parts):
            augment(h, sub, cosine, sine)
        send_margin(0, h)
    if paired:
        for h in range(streams):
            send_margin(1, h)
    for h in range(last):
        step_margin(0, h)
    for sub in range(parts - 1):
        augment(last, sub, cosine, sine)
    if paired:
        for h in range(streams):
            step_margin(1, h)
    augment(last, parts - 1, cosine, sine)
    send_margin(0, last)
    step_margin(0, last)
    drain_waves()
    for h in range(streams):
        real, imag = macc[0, h, 0, 0], macc[0, h, 0, 1]
        if paired:
            real, imag = finish_margin(1, h, real, imag)
        real, imag = finish_margin(0, h, real, imag)
        out[:, 0, columns(h)] = real
        out[:, 1, columns(h)] = imag


def fused(n, kn, order, shift, phase, charges, waves, projectors):
    pw_dev, nb = waves.shape[2], waves.shape[3]
    nproj = projectors.shape[3]
    atoms = phase.shape[1]
    ppa = charges.shape[0]
    rows, share = nproj // n, nb // n
    h = nb // LANES
    parts = pieces_of(rows, ppa)
    zn, half = n // 4, n // 2
    pad = -(-ppa // 8) * 8
    blocks = -(-nproj // (8 * LANES)) * 8
    paired = kn == 2
    unit = pw_dev // 16
    sent_rows = 11 * unit if paired else pw_dev
    slots = 3 if paired else 1
    kinds = 2 if paired else 1
    anywhere = pl.BlockSpec(memory_space=pl.ANY)
    f32, i32, bf16 = jnp.float32, jnp.int32, jnp.bfloat16
    tile = block_of(nproj) if nproj % 256 else 256
    scratch = [
        ((nproj // LANES, LANES), i32), ((1, pw_dev), i32), ((1, atoms), f32), ((ppa, pad, atoms), f32),
        ((blocks, LANES), i32), "smem", ((pw_dev, LANES), i32), ((rows, rows), f32),
        ((2, pw_dev, nb), bf16), ((2, pw_dev, nproj), bf16), ((h, 2, 2 * LANES, pw_dev), bf16),
        ((h, 2 * LANES, nproj), f32), ((h, 2 * LANES, LANES), f32), ((2 * LANES, LANES), f32), ((nproj, LANES), i32),
        ((h, half, rows, LANES), i32), ((h, half, rows, LANES), i32), ((h, half, rows, LANES), i32),
        ((h, 2, LANES), f32), ((h, 2, LANES), f32),
        ((zn, 2, rows // parts, LANES), f32), ((h, zn, rows, LANES), i32), ((h, zn, rows, LANES), i32),
        ((h, parts, 2, LANES), f32), ((h, parts, 2, LANES), f32), ((h, zn, 2, rows, LANES), f32),
        ((h, zn - 1, rows, LANES), i32), ((h, zn - 1, rows, LANES), i32),
        ((h, parts, 2, LANES), f32), ((h, parts, zn - 1, 2, LANES), f32), ((2, rows, nb), f32),
        ((h, rows, LANES), i32), ((h, rows, LANES), i32), ((h, parts, 2, LANES), f32), ((h, parts, 2, LANES), f32),
        ((2, sent_rows, nb), bf16), ((2, sent_rows, nb), bf16), ((2, 5 * unit, nb), bf16),
        ((kinds, 2, nb, nb), f32), ((kinds, h, half, share, LANES), i32), ((kinds, h, half, share, LANES), i32),
        ((kinds, h, 2, LANES), f32), ((kinds, h, 2, LANES), f32), ((kinds, h, half, 2, share, LANES), f32),
        ((kinds, h, half, share, LANES), i32), ((kinds, h, half, share, LANES), i32),
        ((kinds, h, 2, LANES), f32), ((kinds, h, half, 2, LANES), f32),
    ]
    made = [pltpu.SMEM((blocks * LANES,), i32) if s == "smem" else pltpu.VMEM(*s) for s in scratch]
    sems = [
        (nproj // tile + 5 + blocks,), (2, h, parts), (2, h), (2, h, parts, 2), (2, h, parts, zn - 1, 2),
        (2, h, parts, 2), (2, slots), (2, kinds, h, 2), (2, kinds, h, half, 2),
    ]
    return pl.pallas_call(
        functools.partial(fused_kernel, n, kn, ppa),
        out_shape=pltpu.VMEM((share, 2, nb), f32),
        in_specs=[anywhere] * 6,
        out_specs=pl.BlockSpec(memory_space=pltpu.VMEM),
        scratch_shapes=made + [pltpu.SemaphoreType.DMA(s) for s in sems],
        compiler_params=pltpu.CompilerParams(
            collective_id=0, has_side_effects=True, vmem_limit_bytes=62 * 2**20
        ),
    )(order, shift, phase, charges, waves, projectors)


def local(waves, projectors, projector_order, shift_map, charges, atom_phase):
    n = lax.axis_size("pw")
    kn = lax.axis_size("ka")
    summed = fused(
        n, kn, projector_order.reshape(-1, LANES), shift_map[None, :], atom_phase[None, :],
        jnp.transpose(charges, (1, 2, 0)), waves, projectors,
    )
    return summed[None]


def solution(mesh):
    placed = (P("ka", None, "pw", None), P("ka", None, "pw", None), P(), P("pw"), P(), P())
    return jax.shard_map(
        local, mesh=mesh, in_specs=placed, out_specs=P("ka", "pw", None, None), check_vma=False
    )
```

```python
import functools
import math

import jax
import jax.numpy as jnp
from jax import lax
from jax.experimental import pallas as pl
from jax.experimental.pallas import tpu as pltpu
from jax.sharding import PartitionSpec as P

MESH = pl.DeviceIdType.MESH
LANES = 128
TOP = 32767.0
HIGH = lax.Precision.HIGHEST


def dot(left, right, dims, precision=None):
    return lax.dot_general(
        left, right, (((dims[0],), (dims[1],)), ((), ())),
        precision=precision, preferred_element_type=jnp.float32,
    )


def contract(left, right, precision=None):
    return dot(left, right, (0, 0), precision)


def cross(left, right):
    real = contract(left[0], right[0]) + contract(left[1], right[1])
    imag = contract(left[0], right[1]) - contract(left[1], right[0])
    return real, imag


def low(v):
    return jnp.right_shift(jnp.left_shift(v, 16), 16).astype(jnp.float32)


def high(v):
    return jnp.right_shift(v, 16).astype(jnp.float32)


def code(x, inv):
    return jnp.floor(x * inv + 0.5).astype(jnp.int32)


def pack(real, imag, inv_real, inv_imag):
    return jnp.bitwise_or(
        jnp.left_shift(code(imag, inv_imag), 16),
        jnp.bitwise_and(code(real, inv_real), 0xFFFF),
    )


def fold(x):
    return jnp.max(jnp.abs(x).reshape(x.shape[0] // 8, 8, x.shape[1]), axis=0)


def scale_of(top):
    return jnp.maximum(jnp.max(top, axis=0, keepdims=True), 1e-30) * (1.0 / TOP)


def block_of(size):
    for block in (512, 256, 128):
        if size % block == 0:
            return block
    return size


def pieces_of(rows, ppa):
    return 2 if rows % 16 == 0 and (rows // 2) % ppa == 0 else 1


def fused_kernel(
    n, kn, ppa, order_hbm, shift_hbm, phase_hbm, charge_hbm, wave_hbm, beta_hbm, out,
    order, shift, phase, charge, inv_v, inv_s, spread, sym, wave, beta, rhs, proj_t, top, inv_b, packed,
    gs, go, cr, sc0, sc0_r, xf, xs, xr, scx, scx_r, acc, zs, zr, scz, scz_r, mine, ys, yr, scy, scy_r,
    wr, picked, stage, part, ms, mr, scm, scm_r, macc, ds, dr, scd, scd_r,
    local_sems, core_sems, core_scale_sems, x_sems, z_sems, y_sems, wave_sems, m_sems, d_sems,
):
    me = lax.axis_index("pw")
    k = lax.axis_index("ka")
    ahead, behind = lax.rem(k + 1, kn), lax.rem(k + kn - 1, kn)
    last_k = k == kn - 1
    paired = kn == 2
    pw_dev, nb = wave.shape[1], wave.shape[2]
    nproj = beta.shape[2]
    streams = nb // LANES
    rows = gs.shape[2]
    parts = pieces_of(rows, ppa)
    rs = rows // parts
    halfn, zn = n // 2, n // 4
    share = nb // n
    core, xbit, mez, mej = me & 1, (me >> 1) & 1, me >> 2, me >> 1
    tile = block_of(nproj) if nproj % 256 else 256
    tiles = nproj // tile
    unit = pw_dev // 32
    cuts = ((0, 8, 16, 21), (0, 11, 22))
    few = 21 * unit

    def beta_copy(t):
        at = pl.ds(pl.multiple_of(t * tile, tile), tile)
        return pltpu.make_async_copy(beta_hbm.at[0, :, :, at], beta.at[:, :, at], local_sems.at[t])

    small = [
        pltpu.make_async_copy(src, dst, local_sems.at[tiles + i])
        for i, (src, dst) in enumerate((
            (order_hbm, order), (wave_hbm.at[0], wave), (shift_hbm, shift), (phase_hbm, phase),
            (charge_hbm, charge.at[:, pl.ds(0, ppa), :]),
        ))
    ]
    barrier = pltpu.get_barrier_semaphore()
    greet = [{"pw": me ^ 1}, {"pw": me ^ 2}] + [{"pw": me ^ (d << 2)} for d in range(1, zn)]
    greet += [{"ka": ahead}] if paired else [{"ka": ahead}, {"ka": behind}]
    for where in greet:
        pl.semaphore_signal(barrier, inc=1, device_id=where, device_id_type=MESH)

    for copy in small[:2]:
        copy.start()
    depth = min(4, tiles)
    for t in range(depth):
        beta_copy(t).start()
    for copy in small[2:5]:
        copy.start()

    inverse_copies = [
        pltpu.make_async_copy(inv_v.at[b], inv_s.at[pl.ds(b * LANES, LANES)], local_sems.at[tiles + 5 + b])
        for b in range(inv_v.shape[0])
    ]
    def remote(src, dst, send, recv, where):
        return pltpu.make_async_remote_copy(
            src_ref=src, dst_ref=dst, send_sem=send, recv_sem=recv,
            device_id=where, device_id_type=MESH,
        )

    def invert():
        blocks = inv_v.shape[0]
        small[0].wait()
        slots = jnp.concatenate([order[r : r + 1, :] for r in range(nproj // LANES)], axis=1)
        upper, lower = jnp.right_shift(slots, 7), jnp.bitwise_and(slots, 127)
        place = lax.broadcasted_iota(jnp.int32, (1, nproj), 1)
        hot_u = lax.broadcasted_iota(jnp.int32, (blocks, nproj), 0) == upper
        hot_l = lax.broadcasted_iota(jnp.int32, (LANES, nproj), 0) == lower
        coarse = jnp.right_shift(place, 4).astype(jnp.float32)
        fine = jnp.bitwise_and(place, 15).astype(jnp.float32)
        left = jnp.concatenate([jnp.where(hot_u, coarse, 0.0), jnp.where(hot_u, fine, 0.0)], axis=0)
        found = dot(left.astype(jnp.bfloat16), jnp.where(hot_l, 1.0, 0.0).astype(jnp.bfloat16), (1, 1))
        found = (found[:blocks] * 16.0 + found[blocks:] + 0.5).astype(jnp.int32)
        inv_v[...] = jnp.clip(found, 0, nproj - 1)
        for copy in inverse_copies:
            copy.start()

    def transpose_waves():
        small[1].wait()
        for p in range(2):
            flat = wave[p].T
            for h in range(streams):
                mid = flat[h * LANES : (h + 1) * LANES]
                rhs[h, p, :LANES, :] = mid
                rhs[h, 1 - p, LANES:, :] = mid if p else -mid

    def multiply(hs, start, stop):
        def step(t, carry):
            if 0 in hs:
                beta_copy(t).wait()

                @pl.when(t + depth < tiles)
                def _():
                    beta_copy(t + depth).start()

            at = pl.ds(pl.multiple_of(t * tile, tile), tile)
            for h in hs:
                got = dot(rhs[h, 0], beta[0, :, at], (1, 0)) + dot(rhs[h, 1], beta[1, :, at], (1, 0))
                proj_t[h, :, at] = got
                peak = top[h]
                for b in range(tile // LANES):
                    peak = jnp.maximum(peak, jnp.abs(got[:, b * LANES : (b + 1) * LANES]))
                top[h] = peak
            return carry

        lax.fori_loop(start, stop, step, 0)

    def encode(h):
        peak = jnp.max(top[h], axis=1, keepdims=True)
        scale = jnp.maximum(peak, 1e-30) * (1.0 / TOP)
        inv_b[...] = jnp.broadcast_to(1.0 / scale, inv_b.shape)
        flat = jnp.broadcast_to(scale, inv_b.shape)
        sc0[h, 0:1, :] = flat[:LANES].T[0:1]
        sc0[h, 1:2, :] = flat[LANES:].T[0:1]

        def step(t, carry):
            at = pl.ds(pl.multiple_of(t * LANES, LANES), LANES)
            coded = pack(proj_t[h, :LANES, at], proj_t[h, LANES:, at], inv_b[:LANES], inv_b[LANES:])
            packed[at, :] = coded.T
            return carry

        lax.fori_loop(0, nproj // LANES, step, 0, unroll=3)

    def gather(dst, h, parity, sub):
        def one(j, carry):
            base = ((j << 1) | parity) * rows + sub * rs
            for g in range(rs // 8):
                slot = base + 8 * g
                taken = [packed[pl.ds(inv_s[slot + r], 1), :] for r in range(8)]
                dst[h, j, pl.ds(sub * rs + 8 * g, 8), :] = jnp.concatenate(taken, axis=0)
            return carry

        lax.fori_loop(0, halfn, one, 0)

    def span(sub):
        return pl.ds(sub * rs, rs)

    def core_copy(h, sub):
        return remote(
            gs.at[h, :, span(sub)], cr.at[h, :, span(sub)],
            core_sems.at[0, h, sub], core_sems.at[1, h, sub], {"pw": me ^ 1},
        )

    def core_scale_copy(h):
        return remote(sc0.at[h], sc0_r.at[h], core_scale_sems.at[0, h], core_scale_sems.at[1, h], {"pw": me ^ 1})

    def x_copies(h, sub):
        sems, where = x_sems, {"pw": me ^ 2}
        return [
            remote(xs.at[h, :, span(sub)], xr.at[h, :, span(sub)], sems.at[0, h, sub, 0], sems.at[1, h, sub, 0], where),
            remote(scx.at[h, sub], scx_r.at[h, sub], sems.at[0, h, sub, 1], sems.at[1, h, sub, 1], where),
        ]

    def z_copies(h, sub):
        made = []
        for d in range(1, zn):
            where = {"pw": me ^ (d << 2)}
            made.append(remote(
                zs.at[h, d - 1, span(sub)], zr.at[h, d - 1, span(sub)],
                z_sems.at[0, h, sub, d - 1, 0], z_sems.at[1, h, sub, d - 1, 0], where,
            ))
            made.append(remote(
                scz.at[h, sub], scz_r.at[h, sub, d - 1],
                z_sems.at[0, h, sub, d - 1, 1], z_sems.at[1, h, sub, d - 1, 1], where,
            ))
        return made

    def y_copies(h, sub):
        where = {"ka": behind}
        return [
            remote(ys.at[h, span(sub)], yr.at[h, span(sub)], y_sems.at[0, h, sub, 0], y_sems.at[1, h, sub, 0], where),
            remote(scy.at[h, sub], scy_r.at[h, sub], y_sems.at[0, h, sub, 1], y_sems.at[1, h, sub, 1], where),
        ]

    none = jnp.zeros((8, LANES), jnp.float32)

    def put_scale(ref, h, sub, tops):
        scales = [scale_of(t) for t in tops]
        ref[h, sub, 0:1, :] = scales[0]
        ref[h, sub, 1:2, :] = scales[1]
        return [1.0 / s for s in scales]

    def send_core(h, sub):
        gather(gs, h, 1 - core, sub)
        if sub == 0:
            core_scale_copy(h).start()
        core_copy(h, sub).start()

    def step_core(h, sub):
        if sub == 0:
            core_scale_copy(h).wait()
        core_copy(h, sub).wait()
        at = span(sub)
        own_r, own_i = sc0[h, 0:1, :], sc0[h, 1:2, :]
        sib_r, sib_i = sc0_r[h, 0:1, :], sc0_r[h, 1:2, :]

        def total(j):
            a, b = go[h, j, at, :], cr[h, j, at, :]
            return low(a) * own_r + low(b) * sib_r, high(a) * own_i + high(b) * sib_i

        def first(z, carry):
            tr, ti = carry
            real, imag = total((z << 1) | (1 - xbit))
            xf[z, 0], xf[z, 1] = real, imag
            return jnp.maximum(tr, fold(real)), jnp.maximum(ti, fold(imag))

        inv = put_scale(scx, h, sub, lax.fori_loop(0, zn, first, (none, none)))

        def second(z, carry):
            xs[h, z, at, :] = pack(xf[z, 0], xf[z, 1], *inv)
            return carry

        lax.fori_loop(0, zn, second, 0)
        for copy in x_copies(h, sub):
            copy.start()

        def keep(z, carry):
            real, imag = total((z << 1) | xbit)
            acc[h, z, 0, at, :] = real
            acc[h, z, 1, at, :] = imag
            return carry

        lax.fori_loop(0, zn, keep, 0)

    def step_x(h, sub):
        for copy in x_copies(h, sub):
            copy.wait()
        at = span(sub)
        s_r, s_i = scx_r[h, sub, 0:1, :], scx_r[h, sub, 1:2, :]

        def total(z):
            v = xr[h, z, at, :]
            real = acc[h, z, 0, at, :] + low(v) * s_r
            imag = acc[h, z, 1, at, :] + high(v) * s_i
            acc[h, z, 0, at, :] = real
            acc[h, z, 1, at, :] = imag
            return real, imag

        def first(d, carry):
            tr, ti = carry
            real, imag = total(mez ^ d)
            return jnp.maximum(tr, fold(real)), jnp.maximum(ti, fold(imag))

        inv = put_scale(scz, h, sub, lax.fori_loop(1, zn, first, (none, none)))

        def second(d, carry):
            z = mez ^ d
            zs[h, d - 1, at, :] = pack(acc[h, z, 0, at, :], acc[h, z, 1, at, :], *inv)
            return carry

        lax.fori_loop(1, zn, second, 0)
        for copy in z_copies(h, sub):
            copy.start()
        total(mez)

    def step_z(h, sub):
        for copy in z_copies(h, sub):
            copy.wait()
        at = span(sub)
        real, imag = acc[h, mez, 0, at, :], acc[h, mez, 1, at, :]
        for d in range(zn - 1):
            v = zr[h, d, at, :]
            real = real + low(v) * scz_r[h, sub, d, 0:1, :]
            imag = imag + high(v) * scz_r[h, sub, d, 1:2, :]
        cols = slice(h * LANES, (h + 1) * LANES)
        mine[0, at, cols] = real
        mine[1, at, cols] = imag
        inv = put_scale(scy, h, sub, (fold(real), fold(imag)))
        ys[h, at, :] = pack(real, imag, *inv)
        for copy in y_copies(h, sub):
            copy.start()

    def wave_copy(i, src, at):
        return remote(src, wr.at[:, at, :], wave_sems.at[0, i], wave_sems.at[1, i], {"ka": behind})

    def landing(side, i):
        low_end, high_end = cuts[side][i : i + 2]
        return pl.ds(low_end * unit, (high_end - low_end) * unit)

    def sent(side, i):
        if side == 1:
            return wave_copy(i, wave.at[:, landing(0, i), :], landing(0, i))
        src = stage if i else wave.at[:, pl.ds(few, pw_dev - few), :]
        return wave_copy(i, src, landing(1, i))

    def whole_wave():
        return wave_copy(0, wave, pl.ds(0, pw_dev))

    def send_waves():
        if not paired:
            whole_wave().start()
            return

        @pl.when(k == 0)
        def _():
            sent(0, 0).start()

        @pl.when(k == 1)
        def _():
            for i in range(3):
                sent(1, i).start()

    def spread_shift():
        small[2].wait()
        for b in range(pw_dev // LANES):
            line = shift[0:1, b * LANES : (b + 1) * LANES] - me * pw_dev
            spread[pl.ds(b * LANES, LANES), :] = jnp.broadcast_to(line, (LANES, LANES)).T

    def permute(dst, src, start, size, offset):
        block = next((b for b in (256, 192, 320, 352, 128) if size % b == 0), size)

        def step(b, carry):
            at = pl.ds(pl.multiple_of(start + b * block, math.gcd(start, block)), block)
            to = pl.ds(pl.multiple_of(offset + b * block, math.gcd(offset, block)), block)
            want = spread[at, :]
            lane = lax.broadcasted_iota(jnp.int32, (block, LANES), 1)
            hot = jnp.concatenate(
                [jnp.where(want == lane + g * LANES, 1.0, 0.0) for g in range(pw_dev // LANES)], axis=1
            ).astype(jnp.bfloat16)
            for p in range(2):
                dst[p, to, :] = dot(hot, src(p), (1, 0)).astype(jnp.bfloat16)
            return carry

        lax.fori_loop(0, size // block, step, 0)

    def send_picked():
        @pl.when(k == 0)
        def _():
            permute(stage, lambda p: wave[p], few, pw_dev - few, 0)
            sent(0, 1).start()

    def build_picked(i):
        @pl.when(k == 0)
        def _():
            start, stop = cuts[0][i] * unit, cuts[0][i + 1] * unit
            permute(picked, lambda p: wave[p], start, stop - start, start)

    def add(which, values, fresh):
        for c in range(2):
            if fresh:
                part[which, c] = values[c]
            else:
                part[which, c] += values[c]

    def piece(ref, start, stop):
        return [ref[p, start:stop, :] for p in range(2)]

    def plane_first(i):
        @pl.when(k == 0)
        def _():
            sent(1, i).wait_recv()
            ends = cuts[0][i] * unit, cuts[0][i + 1] * unit
            got = piece(wr, *ends)
            add(0, cross(piece(wave, *ends), got), i == 0)
            add(1, cross(got, piece(picked, *ends)), i == 0)

    def plane_second(i):
        @pl.when(k == 1)
        def _():
            sent(0, i).wait_recv()
            got = piece(wr, cuts[1][i] * unit, cuts[1][i + 1] * unit)
            rest = piece(wave, few, pw_dev)
            if i == 0:
                add(1, cross(got, rest), True)
            else:
                add(0, cross(rest, got), True)

    def drain_waves():
        if not paired:
            whole_wave().wait_send()
            return

        @pl.when(k == 0)
        def _():
            for i in range(2):
                sent(0, i).wait_send()

        @pl.when(k == 1)
        def _():
            for i in range(3):
                sent(1, i).wait_send()

    def plane_ring():
        whole_wave().wait_recv()

        @pl.when(last_k)
        def _():
            permute(picked, lambda p: wr[p], 0, pw_dev, 0)

        @pl.when(k != kn - 1)
        def _():
            picked[...] = wr[...]

        add(0, cross([wave[0], wave[1]], [picked[0], picked[1]]), True)

    def make_tables():
        small[3].wait()
        small[4].wait()
        atoms = phase.shape[1]
        own_atoms = rows // ppa
        row_i = lax.broadcasted_iota(jnp.int32, (rows, atoms), 0)
        lane = lax.broadcasted_iota(jnp.int32, (rows, atoms), 1)
        away = row_i - ppa * (lane - me * own_atoms)
        hit = (away >= 0) & (away < ppa)
        angle = jnp.where(last_k, phase[...], 0.0)
        cosine = jnp.sum(jnp.where(hit, jnp.cos(angle), 0.0), axis=1, keepdims=True)
        sine = jnp.sum(jnp.where(hit, jnp.sin(angle), 0.0), axis=1, keepdims=True)
        pad = charge.shape[1]
        flat = charge[...].reshape(ppa * pad, atoms)
        pick = jnp.where(hit, 1.0, 0.0)
        every = dot(pick, flat, (1, 1), HIGH)

        def iota(shape, axis):
            return lax.broadcasted_iota(jnp.int32, shape, axis).astype(jnp.float32)

        def div(x, by):
            return jnp.floor((x + 0.5) * (1.0 / by))

        shape = (rows, ppa * pad)
        r, c = iota(shape, 0), iota(shape, 1)
        own_p = r - ppa * div(r, ppa)
        col_p = div(c, pad)
        kept = jnp.where((own_p == col_p) & (c - pad * col_p < ppa), every, 0.0)
        shape = (ppa * pad, rows)
        c, j = iota(shape, 0), iota(shape, 1)
        widen = jnp.where(c - pad * div(c, pad) == j - ppa * div(j, ppa), 1.0, 0.0)
        full = dot(kept, widen, (1, 0), HIGH) + dot(widen, kept, (0, 1), HIGH)
        shape = (rows, rows)
        same = div(iota(shape, 0), ppa) == div(iota(shape, 1), ppa)
        sym[...] = jnp.where(same, 0.5 * full, 0.0)
        return cosine, sine

    def m_copies(w, h):
        where = {"pw": me ^ 1}
        return [
            remote(ms.at[w, h], mr.at[w, h], m_sems.at[0, w, h, 0], m_sems.at[1, w, h, 0], where),
            remote(scm.at[w, h], scm_r.at[w, h], m_sems.at[0, w, h, 1], m_sems.at[1, w, h, 1], where),
        ]

    def d_copies(w, h):
        made = []
        for d in range(1 - w, halfn):
            where = {"pw": me ^ (d << 1)}
            if w:
                where["ka"] = ahead
            made.append(remote(
                ds.at[w, h, d], dr.at[w, h, d], d_sems.at[0, w, h, d, 0], d_sems.at[1, w, h, d, 0], where,
            ))
            made.append(remote(
                scd.at[w, h], scd_r.at[w, h, d], d_sems.at[0, w, h, d, 1], d_sems.at[1, w, h, d, 1], where,
            ))
        return made

    def block_at(j, parity):
        return pl.ds(pl.multiple_of(((j << 1) | parity) * share, share), share)

    def columns(h):
        return slice(h * LANES, (h + 1) * LANES)

    def send_margin(w, h):
        cols = columns(h)

        def first(j, carry):
            at = block_at(j, 1 - core)
            return (
                jnp.maximum(carry[0], fold(part[w, 0, at, cols])),
                jnp.maximum(carry[1], fold(part[w, 1, at, cols])),
            )

        inv = put_scale(scm, w, h, lax.fori_loop(0, halfn, first, (none, none)))

        def second(j, carry):
            at = block_at(j, 1 - core)
            ms[w, h, j] = pack(part[w, 0, at, cols], part[w, 1, at, cols], *inv)
            return carry

        lax.fori_loop(0, halfn, second, 0)
        for copy in m_copies(w, h):
            copy.start()

    def step_margin(w, h):
        for copy in m_copies(w, h):
            copy.wait()
        cols = columns(h)
        s_r, s_i = scm_r[w, h, 0:1, :], scm_r[w, h, 1:2, :]

        def first(d, carry):
            j = mej ^ d
            at = block_at(j, core)
            v = mr[w, h, j]
            real = part[w, 0, at, cols] + low(v) * s_r
            imag = part[w, 1, at, cols] + high(v) * s_i
            macc[w, h, d, 0], macc[w, h, d, 1] = real, imag
            return jnp.maximum(carry[0], fold(real)), jnp.maximum(carry[1], fold(imag))

        inv = put_scale(scd, w, h, lax.fori_loop(0, halfn, first, (none, none)))

        def second(d, carry):
            ds[w, h, d] = pack(macc[w, h, d, 0], macc[w, h, d, 1], *inv)
            return carry

        lax.fori_loop(1 - w, halfn, second, 0)
        for copy in d_copies(w, h):
            copy.start()

    def finish_margin(w, h, real, imag):
        for copy in d_copies(w, h):
            copy.wait()
        for d in range(1 - w, halfn):
            v = dr[w, h, d]
            real = real + low(v) * scd_r[w, h, d, 0:1, :]
            imag = imag + high(v) * scd_r[w, h, d, 1:2, :]
        return real, imag

    def augment(h, sub, cosine, sine):
        if not paired or h + sub > 0:
            for copy in y_copies(h, sub):
                copy.wait()
        at = slice(sub * rs, (sub + 1) * rs)
        v = yr[h, at, :]
        nr, ni = low(v) * scy_r[h, sub, 0:1, :], high(v) * scy_r[h, sub, 1:2, :]
        c, s = cosine[at], sine[at]
        turned = jnp.concatenate([nr * c + ni * s, ni * c - nr * s], axis=1)
        weighted = dot(sym[at, at], turned, (1, 0), HIGH)
        by_real = contract(mine[0, at, :], weighted, HIGH)
        by_imag = contract(mine[1, at, :], weighted, HIGH)
        cols = columns(h)
        part[0, 0, :, cols] += by_real[:, :LANES] + by_imag[:, LANES:]
        part[0, 1, :, cols] += by_real[:, LANES:] - by_imag[:, :LANES]

    last = streams - 1
    early = tiles // 3
    invert()
    transpose_waves()
    top[...] = jnp.zeros_like(top)
    multiply(range(streams), 0, early)
    pl.semaphore_wait(barrier, len(greet))
    send_waves()
    multiply((0,), early, tiles)
    for h in range(streams):
        if h == last:
            spread_shift()
            if paired:
                send_picked()
        if h > 0:
            multiply((h,), early, tiles)
        encode(h)
        if h == 0:
            for copy in inverse_copies:
                copy.wait()
        for sub in range(parts):
            send_core(h, sub)
        for sub in range(parts):
            gather(go, h, core, sub)
            step_core(h, sub)
            if h > 0:
                step_x(h - 1, sub)
    step_x(last, 0)
    if paired:
        build_picked(0)
        plane_first(0)
        plane_second(0)
    for sub in range(1, parts):
        step_x(last, sub)
    if paired:
        build_picked(1)
        plane_first(1)
    for h in range(last):
        for sub in range(parts):
            step_z(h, sub)
    if paired:
        build_picked(2)
    cosine, sine = make_tables()
    for sub in range(parts - 1):
        step_z(last, sub)
    if paired:
        plane_first(2)
        for h in range(streams):
            send_margin(1, h)
    step_z(last, parts - 1)
    if paired:
        for copy in y_copies(0, 0):
            copy.wait()
        for h in range(streams):
            step_margin(1, h)
        plane_second(1)
    else:
        plane_ring()
    for h in range(last):
        for sub in range(parts):
            augment(h, sub, cosine, sine)
        send_margin(0, h)
    for sub in range(parts - 1):
        augment(last, sub, cosine, sine)
    for h in range(last):
        step_margin(0, h)
    augment(last, parts - 1, cosine, sine)
    send_margin(0, last)
    step_margin(0, last)
    drain_waves()
    for h in range(streams):
        real, imag = macc[0, h, 0, 0], macc[0, h, 0, 1]
        if paired:
            real, imag = finish_margin(1, h, real, imag)
        real, imag = finish_margin(0, h, real, imag)
        out[:, 0, columns(h)] = real
        out[:, 1, columns(h)] = imag


def fused(n, kn, order, shift, phase, charges, waves, projectors):
    pw_dev, nb = waves.shape[2], waves.shape[3]
    nproj = projectors.shape[3]
    atoms = phase.shape[1]
    ppa = charges.shape[0]
    rows, share = nproj // n, nb // n
    h = nb // LANES
    parts = pieces_of(rows, ppa)
    zn, half = n // 4, n // 2
    pad = -(-ppa // 8) * 8
    blocks = -(-nproj // (8 * LANES)) * 8
    paired = kn == 2
    unit = pw_dev // 32
    sent_rows = 22 * unit if paired else pw_dev
    slots = 3 if paired else 1
    kinds = 2 if paired else 1
    anywhere = pl.BlockSpec(memory_space=pl.ANY)
    f32, i32, bf16 = jnp.float32, jnp.int32, jnp.bfloat16
    tile = block_of(nproj) if nproj % 256 else 256
    scratch = [
        ((nproj // LANES, LANES), i32), ((1, pw_dev), i32), ((1, atoms), f32), ((ppa, pad, atoms), f32),
        ((blocks, LANES), i32), "smem", ((pw_dev, LANES), i32), ((rows, rows), f32),
        ((2, pw_dev, nb), bf16), ((2, pw_dev, nproj), bf16), ((h, 2, 2 * LANES, pw_dev), bf16),
        ((h, 2 * LANES, nproj), f32), ((h, 2 * LANES, LANES), f32), ((2 * LANES, LANES), f32), ((nproj, LANES), i32),
        ((h, half, rows, LANES), i32), ((h, half, rows, LANES), i32), ((h, half, rows, LANES), i32),
        ((h, 2, LANES), f32), ((h, 2, LANES), f32),
        ((zn, 2, rows // parts, LANES), f32), ((h, zn, rows, LANES), i32), ((h, zn, rows, LANES), i32),
        ((h, parts, 2, LANES), f32), ((h, parts, 2, LANES), f32), ((h, zn, 2, rows, LANES), f32),
        ((h, zn - 1, rows, LANES), i32), ((h, zn - 1, rows, LANES), i32),
        ((h, parts, 2, LANES), f32), ((h, parts, zn - 1, 2, LANES), f32), ((2, rows, nb), f32),
        ((h, rows, LANES), i32), ((h, rows, LANES), i32), ((h, parts, 2, LANES), f32), ((h, parts, 2, LANES), f32),
        ((2, sent_rows, nb), bf16), ((2, sent_rows, nb), bf16), ((2, 11 * unit, nb), bf16),
        ((kinds, 2, nb, nb), f32), ((kinds, h, half, share, LANES), i32), ((kinds, h, half, share, LANES), i32),
        ((kinds, h, 2, LANES), f32), ((kinds, h, 2, LANES), f32), ((kinds, h, half, 2, share, LANES), f32),
        ((kinds, h, half, share, LANES), i32), ((kinds, h, half, share, LANES), i32),
        ((kinds, h, 2, LANES), f32), ((kinds, h, half, 2, LANES), f32),
    ]
    made = [pltpu.SMEM((blocks * LANES,), i32) if s == "smem" else pltpu.VMEM(*s) for s in scratch]
    sems = [
        (nproj // tile + 5 + blocks,), (2, h, parts), (2, h), (2, h, parts, 2), (2, h, parts, zn - 1, 2),
        (2, h, parts, 2), (2, slots), (2, kinds, h, 2), (2, kinds, h, half, 2),
    ]
    return pl.pallas_call(
        functools.partial(fused_kernel, n, kn, ppa),
        out_shape=pltpu.VMEM((share, 2, nb), f32),
        in_specs=[anywhere] * 6,
        out_specs=pl.BlockSpec(memory_space=pltpu.VMEM),
        scratch_shapes=made + [pltpu.SemaphoreType.DMA(s) for s in sems],
        compiler_params=pltpu.CompilerParams(
            collective_id=0, has_side_effects=True, vmem_limit_bytes=62 * 2**20
        ),
    )(order, shift, phase, charges, waves, projectors)


def local(waves, projectors, projector_order, shift_map, charges, atom_phase):
    n = lax.axis_size("pw")
    kn = lax.axis_size("ka")
    summed = fused(
        n, kn, projector_order.reshape(-1, LANES), shift_map[None, :], atom_phase[None, :],
        jnp.transpose(charges, (1, 2, 0)), waves, projectors,
    )
    return summed[None]


def solution(mesh):
    placed = (P("ka", None, "pw", None), P("ka", None, "pw", None), P(), P("pw"), P(), P())
    return jax.shard_map(
        local, mesh=mesh, in_specs=placed, out_specs=P("ka", "pw", None, None), check_vma=False
    )
```

```python
import functools
import math

import jax
import jax.numpy as jnp
from jax import lax
from jax.experimental import pallas as pl
from jax.experimental.pallas import tpu as pltpu
from jax.sharding import PartitionSpec as P

MESH = pl.DeviceIdType.MESH
LANES = 128
TOP = 32767.0
HIGH = lax.Precision.HIGHEST


def dot(left, right, dims, precision=None):
    return lax.dot_general(
        left, right, (((dims[0],), (dims[1],)), ((), ())),
        precision=precision, preferred_element_type=jnp.float32,
    )


def contract(left, right, precision=None):
    return dot(left, right, (0, 0), precision)


def cross(left, right):
    real = contract(left[0], right[0]) + contract(left[1], right[1])
    imag = contract(left[0], right[1]) - contract(left[1], right[0])
    return real, imag


def low(v):
    return jnp.right_shift(jnp.left_shift(v, 16), 16).astype(jnp.float32)


def high(v):
    return jnp.right_shift(v, 16).astype(jnp.float32)


def code(x, inv):
    return jnp.floor(x * inv + 0.5).astype(jnp.int32)


def pack(real, imag, inv_real, inv_imag):
    return jnp.bitwise_or(
        jnp.left_shift(code(imag, inv_imag), 16),
        jnp.bitwise_and(code(real, inv_real), 0xFFFF),
    )


def fold(x):
    return jnp.max(jnp.abs(x).reshape(x.shape[0] // 8, 8, x.shape[1]), axis=0)


def scale_of(top):
    return jnp.maximum(jnp.max(top, axis=0, keepdims=True), 1e-30) * (1.0 / TOP)


def block_of(size):
    for block in (512, 256, 128):
        if size % block == 0:
            return block
    return size


def pieces_of(rows, ppa):
    return 2 if rows % 16 == 0 and (rows // 2) % ppa == 0 else 1


def fused_kernel(
    n, kn, ppa, order_hbm, shift_hbm, phase_hbm, charge_hbm, wave_hbm, beta_hbm, out,
    order, shift, phase, charge, inv_v, inv_s, spread, sym, wave, beta, rhs, proj_t, top, inv_b, packed,
    gs, go, cr, sc0, sc0_r, xf, xs, xr, scx, scx_r, acc, zs, zr, scz, scz_r, mine, ys, yr, scy, scy_r,
    wr, picked, stage, part, ms, mr, scm, scm_r, macc, ds, dr, scd, scd_r,
    local_sems, core_sems, core_scale_sems, x_sems, z_sems, y_sems, wave_sems, m_sems, d_sems,
):
    me = lax.axis_index("pw")
    k = lax.axis_index("ka")
    ahead, behind = lax.rem(k + 1, kn), lax.rem(k + kn - 1, kn)
    last_k = k == kn - 1
    paired = kn == 2
    pw_dev, nb = wave.shape[1], wave.shape[2]
    nproj = beta.shape[2]
    streams = nb // LANES
    rows = gs.shape[2]
    parts = pieces_of(rows, ppa)
    rs = rows // parts
    halfn, zn = n // 2, n // 4
    share = nb // n
    core, xbit, mez, mej = me & 1, (me >> 1) & 1, me >> 2, me >> 1
    tile = block_of(nproj) if nproj % 256 else 256
    tiles = nproj // tile
    unit = pw_dev // 32
    cuts = ((0, 8, 16, 21), (0, 11, 22))
    few = 21 * unit

    def beta_copy(t):
        at = pl.ds(pl.multiple_of(t * tile, tile), tile)
        return pltpu.make_async_copy(beta_hbm.at[0, :, :, at], beta.at[:, :, at], local_sems.at[t])

    small = [
        pltpu.make_async_copy(src, dst, local_sems.at[tiles + i])
        for i, (src, dst) in enumerate((
            (order_hbm, order), (wave_hbm.at[0], wave), (shift_hbm, shift), (phase_hbm, phase),
            (charge_hbm, charge.at[:, pl.ds(0, ppa), :]),
        ))
    ]
    barrier = pltpu.get_barrier_semaphore()
    greet = [{"pw": me ^ 1}, {"pw": me ^ 2}] + [{"pw": me ^ (d << 2)} for d in range(1, zn)]
    greet += [{"ka": ahead}] if paired else [{"ka": ahead}, {"ka": behind}]
    for where in greet:
        pl.semaphore_signal(barrier, inc=1, device_id=where, device_id_type=MESH)

    for copy in small[:2]:
        copy.start()
    depth = min(4, tiles)
    for t in range(depth):
        beta_copy(t).start()
    for copy in small[2:5]:
        copy.start()

    inverse_copies = [
        pltpu.make_async_copy(inv_v.at[b], inv_s.at[pl.ds(b * LANES, LANES)], local_sems.at[tiles + 5 + b])
        for b in range(inv_v.shape[0])
    ]
    def remote(src, dst, send, recv, where):
        return pltpu.make_async_remote_copy(
            src_ref=src, dst_ref=dst, send_sem=send, recv_sem=recv,
            device_id=where, device_id_type=MESH,
        )

    def invert():
        blocks = inv_v.shape[0]
        small[0].wait()
        slots = jnp.concatenate([order[r : r + 1, :] for r in range(nproj // LANES)], axis=1)
        upper, lower = jnp.right_shift(slots, 7), jnp.bitwise_and(slots, 127)
        place = lax.broadcasted_iota(jnp.int32, (1, nproj), 1)
        hot_u = lax.broadcasted_iota(jnp.int32, (blocks, nproj), 0) == upper
        hot_l = lax.broadcasted_iota(jnp.int32, (LANES, nproj), 0) == lower
        coarse = jnp.right_shift(place, 4).astype(jnp.float32)
        fine = jnp.bitwise_and(place, 15).astype(jnp.float32)
        left = jnp.concatenate([jnp.where(hot_u, coarse, 0.0), jnp.where(hot_u, fine, 0.0)], axis=0)
        found = dot(left.astype(jnp.bfloat16), jnp.where(hot_l, 1.0, 0.0).astype(jnp.bfloat16), (1, 1))
        found = (found[:blocks] * 16.0 + found[blocks:] + 0.5).astype(jnp.int32)
        inv_v[...] = jnp.clip(found, 0, nproj - 1)
        for copy in inverse_copies:
            copy.start()

    def transpose_waves():
        small[1].wait()
        for p in range(2):
            flat = wave[p].T
            for h in range(streams):
                mid = flat[h * LANES : (h + 1) * LANES]
                rhs[h, p, :LANES, :] = mid
                rhs[h, 1 - p, LANES:, :] = mid if p else -mid

    def multiply(hs, start, stop):
        def step(t, carry):
            if 0 in hs:
                beta_copy(t).wait()

                @pl.when(t + depth < tiles)
                def _():
                    beta_copy(t + depth).start()

            at = pl.ds(pl.multiple_of(t * tile, tile), tile)
            for h in hs:
                got = dot(rhs[h, 0], beta[0, :, at], (1, 0)) + dot(rhs[h, 1], beta[1, :, at], (1, 0))
                proj_t[h, :, at] = got
                peak = top[h]
                for b in range(tile // LANES):
                    peak = jnp.maximum(peak, jnp.abs(got[:, b * LANES : (b + 1) * LANES]))
                top[h] = peak
            return carry

        lax.fori_loop(start, stop, step, 0)

    def encode(h):
        peak = jnp.max(top[h], axis=1, keepdims=True)
        scale = jnp.maximum(peak, 1e-30) * (1.0 / TOP)
        inv_b[...] = jnp.broadcast_to(1.0 / scale, inv_b.shape)
        flat = jnp.broadcast_to(scale, inv_b.shape)
        sc0[h, 0:1, :] = flat[:LANES].T[0:1]
        sc0[h, 1:2, :] = flat[LANES:].T[0:1]

        def step(t, carry):
            at = pl.ds(pl.multiple_of(t * LANES, LANES), LANES)
            coded = pack(proj_t[h, :LANES, at], proj_t[h, LANES:, at], inv_b[:LANES], inv_b[LANES:])
            packed[at, :] = coded.T
            return carry

        lax.fori_loop(0, nproj // LANES, step, 0, unroll=3)

    def gather(dst, h, parity, sub):
        def one(j, carry):
            base = ((j << 1) | parity) * rows + sub * rs
            for g in range(rs // 8):
                slot = base + 8 * g
                taken = [packed[pl.ds(inv_s[slot + r], 1), :] for r in range(8)]
                dst[h, j, pl.ds(sub * rs + 8 * g, 8), :] = jnp.concatenate(taken, axis=0)
            return carry

        lax.fori_loop(0, halfn, one, 0)

    def span(sub):
        return pl.ds(sub * rs, rs)

    def core_copy(h, sub):
        return remote(
            gs.at[h, :, span(sub)], cr.at[h, :, span(sub)],
            core_sems.at[0, h, sub], core_sems.at[1, h, sub], {"pw": me ^ 1},
        )

    def core_scale_copy(h):
        return remote(sc0.at[h], sc0_r.at[h], core_scale_sems.at[0, h], core_scale_sems.at[1, h], {"pw": me ^ 1})

    def x_copies(h, sub):
        sems, where = x_sems, {"pw": me ^ 2}
        return [
            remote(xs.at[h, :, span(sub)], xr.at[h, :, span(sub)], sems.at[0, h, sub, 0], sems.at[1, h, sub, 0], where),
            remote(scx.at[h, sub], scx_r.at[h, sub], sems.at[0, h, sub, 1], sems.at[1, h, sub, 1], where),
        ]

    def z_copies(h, sub):
        made = []
        for d in range(1, zn):
            where = {"pw": me ^ (d << 2)}
            made.append(remote(
                zs.at[h, d - 1, span(sub)], zr.at[h, d - 1, span(sub)],
                z_sems.at[0, h, sub, d - 1, 0], z_sems.at[1, h, sub, d - 1, 0], where,
            ))
            made.append(remote(
                scz.at[h, sub], scz_r.at[h, sub, d - 1],
                z_sems.at[0, h, sub, d - 1, 1], z_sems.at[1, h, sub, d - 1, 1], where,
            ))
        return made

    def y_copies(h, sub):
        where = {"ka": behind}
        return [
            remote(ys.at[h, span(sub)], yr.at[h, span(sub)], y_sems.at[0, h, sub, 0], y_sems.at[1, h, sub, 0], where),
            remote(scy.at[h, sub], scy_r.at[h, sub], y_sems.at[0, h, sub, 1], y_sems.at[1, h, sub, 1], where),
        ]

    none = jnp.zeros((8, LANES), jnp.float32)

    def put_scale(ref, h, sub, tops):
        scales = [scale_of(t) for t in tops]
        ref[h, sub, 0:1, :] = scales[0]
        ref[h, sub, 1:2, :] = scales[1]
        return [1.0 / s for s in scales]

    def send_core(h, sub):
        gather(gs, h, 1 - core, sub)
        if sub == 0:
            core_scale_copy(h).start()
        core_copy(h, sub).start()

    def step_core(h, sub):
        if sub == 0:
            core_scale_copy(h).wait()
        core_copy(h, sub).wait()
        at = span(sub)
        own_r, own_i = sc0[h, 0:1, :], sc0[h, 1:2, :]
        sib_r, sib_i = sc0_r[h, 0:1, :], sc0_r[h, 1:2, :]

        def total(j):
            a, b = go[h, j, at, :], cr[h, j, at, :]
            return low(a) * own_r + low(b) * sib_r, high(a) * own_i + high(b) * sib_i

        def first(z, carry):
            tr, ti = carry
            real, imag = total((z << 1) | (1 - xbit))
            xf[z, 0], xf[z, 1] = real, imag
            return jnp.maximum(tr, fold(real)), jnp.maximum(ti, fold(imag))

        inv = put_scale(scx, h, sub, lax.fori_loop(0, zn, first, (none, none)))

        def second(z, carry):
            xs[h, z, at, :] = pack(xf[z, 0], xf[z, 1], *inv)
            return carry

        lax.fori_loop(0, zn, second, 0)
        for copy in x_copies(h, sub):
            copy.start()

        def keep(z, carry):
            real, imag = total((z << 1) | xbit)
            acc[h, z, 0, at, :] = real
            acc[h, z, 1, at, :] = imag
            return carry

        lax.fori_loop(0, zn, keep, 0)

    def step_x(h, sub):
        for copy in x_copies(h, sub):
            copy.wait()
        at = span(sub)
        s_r, s_i = scx_r[h, sub, 0:1, :], scx_r[h, sub, 1:2, :]

        def total(z):
            v = xr[h, z, at, :]
            real = acc[h, z, 0, at, :] + low(v) * s_r
            imag = acc[h, z, 1, at, :] + high(v) * s_i
            acc[h, z, 0, at, :] = real
            acc[h, z, 1, at, :] = imag
            return real, imag

        def first(d, carry):
            tr, ti = carry
            real, imag = total(mez ^ d)
            return jnp.maximum(tr, fold(real)), jnp.maximum(ti, fold(imag))

        inv = put_scale(scz, h, sub, lax.fori_loop(1, zn, first, (none, none)))

        def second(d, carry):
            z = mez ^ d
            zs[h, d - 1, at, :] = pack(acc[h, z, 0, at, :], acc[h, z, 1, at, :], *inv)
            return carry

        lax.fori_loop(1, zn, second, 0)
        for copy in z_copies(h, sub):
            copy.start()
        total(mez)

    def step_z(h, sub):
        for copy in z_copies(h, sub):
            copy.wait()
        at = span(sub)
        real, imag = acc[h, mez, 0, at, :], acc[h, mez, 1, at, :]
        for d in range(zn - 1):
            v = zr[h, d, at, :]
            real = real + low(v) * scz_r[h, sub, d, 0:1, :]
            imag = imag + high(v) * scz_r[h, sub, d, 1:2, :]
        cols = slice(h * LANES, (h + 1) * LANES)
        mine[0, at, cols] = real
        mine[1, at, cols] = imag
        inv = put_scale(scy, h, sub, (fold(real), fold(imag)))
        ys[h, at, :] = pack(real, imag, *inv)
        for copy in y_copies(h, sub):
            copy.start()

    def wave_copy(i, src, at):
        return remote(src, wr.at[:, at, :], wave_sems.at[0, i], wave_sems.at[1, i], {"ka": behind})

    def landing(side, i):
        low_end, high_end = cuts[side][i : i + 2]
        return pl.ds(low_end * unit, (high_end - low_end) * unit)

    def sent(side, i):
        if side == 1:
            return wave_copy(i, wave.at[:, landing(0, i), :], landing(0, i))
        src = stage if i else wave.at[:, pl.ds(few, pw_dev - few), :]
        return wave_copy(i, src, landing(1, i))

    def whole_wave():
        return wave_copy(0, wave, pl.ds(0, pw_dev))

    def send_waves():
        if not paired:
            whole_wave().start()
            return

        @pl.when(k == 0)
        def _():
            sent(0, 0).start()

        @pl.when(k == 1)
        def _():
            for i in range(3):
                sent(1, i).start()

    def spread_shift():
        small[2].wait()
        for b in range(pw_dev // LANES):
            line = shift[0:1, b * LANES : (b + 1) * LANES] - me * pw_dev
            spread[pl.ds(b * LANES, LANES), :] = jnp.broadcast_to(line, (LANES, LANES)).T

    def permute(dst, src, start, size, offset):
        block = next((b for b in (256, 192, 320, 352, 128) if size % b == 0), size)

        def step(b, carry):
            at = pl.ds(pl.multiple_of(start + b * block, math.gcd(start, block)), block)
            to = pl.ds(pl.multiple_of(offset + b * block, math.gcd(offset, block)), block)
            want = spread[at, :]
            lane = lax.broadcasted_iota(jnp.int32, (block, LANES), 1)
            hot = jnp.concatenate(
                [jnp.where(want == lane + g * LANES, 1.0, 0.0) for g in range(pw_dev // LANES)], axis=1
            ).astype(jnp.bfloat16)
            for p in range(2):
                dst[p, to, :] = dot(hot, src(p), (1, 0)).astype(jnp.bfloat16)
            return carry

        lax.fori_loop(0, size // block, step, 0)

    def send_picked():
        @pl.when(k == 0)
        def _():
            permute(stage, lambda p: wave[p], few, pw_dev - few, 0)
            sent(0, 1).start()

    def build_picked(i):
        @pl.when(k == 0)
        def _():
            start, stop = cuts[0][i] * unit, cuts[0][i + 1] * unit
            permute(picked, lambda p: wave[p], start, stop - start, start)

    def add(which, values, fresh):
        for c in range(2):
            if fresh:
                part[which, c] = values[c]
            else:
                part[which, c] += values[c]

    def piece(ref, start, stop):
        return [ref[p, start:stop, :] for p in range(2)]

    def plane_first(i):
        @pl.when(k == 0)
        def _():
            sent(1, i).wait_recv()
            ends = cuts[0][i] * unit, cuts[0][i + 1] * unit
            got = piece(wr, *ends)
            add(0, cross(piece(wave, *ends), got), i == 0)
            add(1, cross(got, piece(picked, *ends)), i == 0)

    def plane_second(i):
        @pl.when(k == 1)
        def _():
            sent(0, i).wait_recv()
            got = piece(wr, cuts[1][i] * unit, cuts[1][i + 1] * unit)
            rest = piece(wave, few, pw_dev)
            if i == 0:
                add(1, cross(got, rest), True)
            else:
                add(0, cross(rest, got), True)

    def drain_waves():
        if not paired:
            whole_wave().wait_send()
            return

        @pl.when(k == 0)
        def _():
            for i in range(2):
                sent(0, i).wait_send()

        @pl.when(k == 1)
        def _():
            for i in range(3):
                sent(1, i).wait_send()

    def plane_ring():
        whole_wave().wait_recv()

        @pl.when(last_k)
        def _():
            permute(picked, lambda p: wr[p], 0, pw_dev, 0)

        @pl.when(k != kn - 1)
        def _():
            picked[...] = wr[...]

        add(0, cross([wave[0], wave[1]], [picked[0], picked[1]]), True)

    def make_tables():
        small[3].wait()
        small[4].wait()
        atoms = phase.shape[1]
        own_atoms = rows // ppa
        row_i = lax.broadcasted_iota(jnp.int32, (rows, atoms), 0)
        lane = lax.broadcasted_iota(jnp.int32, (rows, atoms), 1)
        away = row_i - ppa * (lane - me * own_atoms)
        hit = (away >= 0) & (away < ppa)
        angle = jnp.where(last_k, phase[...], 0.0)
        cosine = jnp.sum(jnp.where(hit, jnp.cos(angle), 0.0), axis=1, keepdims=True)
        sine = jnp.sum(jnp.where(hit, jnp.sin(angle), 0.0), axis=1, keepdims=True)
        pad = charge.shape[1]
        flat = charge[...].reshape(ppa * pad, atoms)
        pick = jnp.where(hit, 1.0, 0.0)
        every = dot(pick, flat, (1, 1), HIGH)

        def iota(shape, axis):
            return lax.broadcasted_iota(jnp.int32, shape, axis).astype(jnp.float32)

        def div(x, by):
            return jnp.floor((x + 0.5) * (1.0 / by))

        shape = (rows, ppa * pad)
        r, c = iota(shape, 0), iota(shape, 1)
        own_p = r - ppa * div(r, ppa)
        col_p = div(c, pad)
        kept = jnp.where((own_p == col_p) & (c - pad * col_p < ppa), every, 0.0)
        shape = (ppa * pad, rows)
        c, j = iota(shape, 0), iota(shape, 1)
        widen = jnp.where(c - pad * div(c, pad) == j - ppa * div(j, ppa), 1.0, 0.0)
        full = dot(kept, widen, (1, 0), HIGH) + dot(widen, kept, (0, 1), HIGH)
        shape = (rows, rows)
        same = div(iota(shape, 0), ppa) == div(iota(shape, 1), ppa)
        sym[...] = jnp.where(same, 0.5 * full, 0.0)
        return cosine, sine

    def m_copies(w, h):
        where = {"pw": me ^ 1}
        return [
            remote(ms.at[w, h], mr.at[w, h], m_sems.at[0, w, h, 0], m_sems.at[1, w, h, 0], where),
            remote(scm.at[w, h], scm_r.at[w, h], m_sems.at[0, w, h, 1], m_sems.at[1, w, h, 1], where),
        ]

    def d_copies(w, h):
        made = []
        for d in range(1 - w, halfn):
            where = {"pw": me ^ (d << 1)}
            if w:
                where["ka"] = ahead
            made.append(remote(
                ds.at[w, h, d], dr.at[w, h, d], d_sems.at[0, w, h, d, 0], d_sems.at[1, w, h, d, 0], where,
            ))
            made.append(remote(
                scd.at[w, h], scd_r.at[w, h, d], d_sems.at[0, w, h, d, 1], d_sems.at[1, w, h, d, 1], where,
            ))
        return made

    def block_at(j, parity):
        return pl.ds(pl.multiple_of(((j << 1) | parity) * share, share), share)

    def columns(h):
        return slice(h * LANES, (h + 1) * LANES)

    def send_margin(w, h):
        cols = columns(h)

        def first(j, carry):
            at = block_at(j, 1 - core)
            return (
                jnp.maximum(carry[0], fold(part[w, 0, at, cols])),
                jnp.maximum(carry[1], fold(part[w, 1, at, cols])),
            )

        inv = put_scale(scm, w, h, lax.fori_loop(0, halfn, first, (none, none)))

        def second(j, carry):
            at = block_at(j, 1 - core)
            ms[w, h, j] = pack(part[w, 0, at, cols], part[w, 1, at, cols], *inv)
            return carry

        lax.fori_loop(0, halfn, second, 0)
        for copy in m_copies(w, h):
            copy.start()

    def step_margin(w, h):
        for copy in m_copies(w, h):
            copy.wait()
        cols = columns(h)
        s_r, s_i = scm_r[w, h, 0:1, :], scm_r[w, h, 1:2, :]

        def first(d, carry):
            j = mej ^ d
            at = block_at(j, core)
            v = mr[w, h, j]
            real = part[w, 0, at, cols] + low(v) * s_r
            imag = part[w, 1, at, cols] + high(v) * s_i
            macc[w, h, d, 0], macc[w, h, d, 1] = real, imag
            return jnp.maximum(carry[0], fold(real)), jnp.maximum(carry[1], fold(imag))

        inv = put_scale(scd, w, h, lax.fori_loop(0, halfn, first, (none, none)))

        def second(d, carry):
            ds[w, h, d] = pack(macc[w, h, d, 0], macc[w, h, d, 1], *inv)
            return carry

        lax.fori_loop(1 - w, halfn, second, 0)
        for copy in d_copies(w, h):
            copy.start()

    def finish_margin(w, h, real, imag):
        for copy in d_copies(w, h):
            copy.wait()
        for d in range(1 - w, halfn):
            v = dr[w, h, d]
            real = real + low(v) * scd_r[w, h, d, 0:1, :]
            imag = imag + high(v) * scd_r[w, h, d, 1:2, :]
        return real, imag

    def augment(h, sub, cosine, sine):
        if not paired or h + sub > 0:
            for copy in y_copies(h, sub):
                copy.wait()
        at = slice(sub * rs, (sub + 1) * rs)
        v = yr[h, at, :]
        nr, ni = low(v) * scy_r[h, sub, 0:1, :], high(v) * scy_r[h, sub, 1:2, :]
        c, s = cosine[at], sine[at]
        turned = jnp.concatenate([nr * c + ni * s, ni * c - nr * s], axis=1)
        weighted = dot(sym[at, at], turned, (1, 0), HIGH)
        by_real = contract(mine[0, at, :], weighted, HIGH)
        by_imag = contract(mine[1, at, :], weighted, HIGH)
        cols = columns(h)
        part[0, 0, :, cols] += by_real[:, :LANES] + by_imag[:, LANES:]
        part[0, 1, :, cols] += by_real[:, LANES:] - by_imag[:, :LANES]

    last = streams - 1
    early = tiles // 3
    invert()
    transpose_waves()
    top[...] = jnp.zeros_like(top)
    multiply(range(streams), 0, early)
    pl.semaphore_wait(barrier, len(greet))
    send_waves()
    multiply((0,), early, tiles)
    for h in range(streams):
        if h == last:
            if streams == 1:
                spread_shift()
            if paired:
                send_picked()
        if h > 0:
            multiply((h,), early, tiles)
        encode(h)
        if h == 0:
            for copy in inverse_copies:
                copy.wait()
        for sub in range(parts):
            send_core(h, sub)
        for sub in range(parts):
            gather(go, h, core, sub)
            if h + sub == 0 and streams > 1:
                spread_shift()
            step_core(h, sub)
            if h > 0:
                step_x(h - 1, sub)
    step_x(last, 0)
    if paired:
        build_picked(0)
        plane_first(0)
        plane_second(0)
    for sub in range(1, parts):
        step_x(last, sub)
    if paired:
        build_picked(1)
        plane_first(1)
    for h in range(last):
        for sub in range(parts):
            step_z(h, sub)
    if paired:
        build_picked(2)
    cosine, sine = make_tables()
    for sub in range(parts - 1):
        step_z(last, sub)
    if paired:
        plane_first(2)
        for h in range(streams):
            send_margin(1, h)
    step_z(last, parts - 1)
    if paired:
        for copy in y_copies(0, 0):
            copy.wait()
        for h in range(streams):
            step_margin(1, h)
        plane_second(1)
    else:
        plane_ring()
    for h in range(last):
        for sub in range(parts):
            augment(h, sub, cosine, sine)
        send_margin(0, h)
    for sub in range(parts - 1):
        augment(last, sub, cosine, sine)
    for h in range(last):
        step_margin(0, h)
    augment(last, parts - 1, cosine, sine)
    send_margin(0, last)
    step_margin(0, last)
    drain_waves()
    for h in range(streams):
        real, imag = macc[0, h, 0, 0], macc[0, h, 0, 1]
        if paired:
            real, imag = finish_margin(1, h, real, imag)
        real, imag = finish_margin(0, h, real, imag)
        out[:, 0, columns(h)] = real
        out[:, 1, columns(h)] = imag


def fused(n, kn, order, shift, phase, charges, waves, projectors):
    pw_dev, nb = waves.shape[2], waves.shape[3]
    nproj = projectors.shape[3]
    atoms = phase.shape[1]
    ppa = charges.shape[0]
    rows, share = nproj // n, nb // n
    h = nb // LANES
    parts = pieces_of(rows, ppa)
    zn, half = n // 4, n // 2
    pad = -(-ppa // 8) * 8
    blocks = -(-nproj // (8 * LANES)) * 8
    paired = kn == 2
    unit = pw_dev // 32
    sent_rows = 22 * unit if paired else pw_dev
    slots = 3 if paired else 1
    kinds = 2 if paired else 1
    anywhere = pl.BlockSpec(memory_space=pl.ANY)
    f32, i32, bf16 = jnp.float32, jnp.int32, jnp.bfloat16
    tile = block_of(nproj) if nproj % 256 else 256
    scratch = [
        ((nproj // LANES, LANES), i32), ((1, pw_dev), i32), ((1, atoms), f32), ((ppa, pad, atoms), f32),
        ((blocks, LANES), i32), "smem", ((pw_dev, LANES), i32), ((rows, rows), f32),
        ((2, pw_dev, nb), bf16), ((2, pw_dev, nproj), bf16), ((h, 2, 2 * LANES, pw_dev), bf16),
        ((h, 2 * LANES, nproj), f32), ((h, 2 * LANES, LANES), f32), ((2 * LANES, LANES), f32), ((nproj, LANES), i32),
        ((h, half, rows, LANES), i32), ((h, half, rows, LANES), i32), ((h, half, rows, LANES), i32),
        ((h, 2, LANES), f32), ((h, 2, LANES), f32),
        ((zn, 2, rows // parts, LANES), f32), ((h, zn, rows, LANES), i32), ((h, zn, rows, LANES), i32),
        ((h, parts, 2, LANES), f32), ((h, parts, 2, LANES), f32), ((h, zn, 2, rows, LANES), f32),
        ((h, zn - 1, rows, LANES), i32), ((h, zn - 1, rows, LANES), i32),
        ((h, parts, 2, LANES), f32), ((h, parts, zn - 1, 2, LANES), f32), ((2, rows, nb), f32),
        ((h, rows, LANES), i32), ((h, rows, LANES), i32), ((h, parts, 2, LANES), f32), ((h, parts, 2, LANES), f32),
        ((2, sent_rows, nb), bf16), ((2, sent_rows, nb), bf16), ((2, 11 * unit, nb), bf16),
        ((kinds, 2, nb, nb), f32), ((kinds, h, half, share, LANES), i32), ((kinds, h, half, share, LANES), i32),
        ((kinds, h, 2, LANES), f32), ((kinds, h, 2, LANES), f32), ((kinds, h, half, 2, share, LANES), f32),
        ((kinds, h, half, share, LANES), i32), ((kinds, h, half, share, LANES), i32),
        ((kinds, h, 2, LANES), f32), ((kinds, h, half, 2, LANES), f32),
    ]
    made = [pltpu.SMEM((blocks * LANES,), i32) if s == "smem" else pltpu.VMEM(*s) for s in scratch]
    sems = [
        (nproj // tile + 5 + blocks,), (2, h, parts), (2, h), (2, h, parts, 2), (2, h, parts, zn - 1, 2),
        (2, h, parts, 2), (2, slots), (2, kinds, h, 2), (2, kinds, h, half, 2),
    ]
    return pl.pallas_call(
        functools.partial(fused_kernel, n, kn, ppa),
        out_shape=pltpu.VMEM((share, 2, nb), f32),
        in_specs=[anywhere] * 6,
        out_specs=pl.BlockSpec(memory_space=pltpu.VMEM),
        scratch_shapes=made + [pltpu.SemaphoreType.DMA(s) for s in sems],
        compiler_params=pltpu.CompilerParams(
            collective_id=0, has_side_effects=True, vmem_limit_bytes=62 * 2**20
        ),
    )(order, shift, phase, charges, waves, projectors)


def local(waves, projectors, projector_order, shift_map, charges, atom_phase):
    n = lax.axis_size("pw")
    kn = lax.axis_size("ka")
    summed = fused(
        n, kn, projector_order.reshape(-1, LANES), shift_map[None, :], atom_phase[None, :],
        jnp.transpose(charges, (1, 2, 0)), waves, projectors,
    )
    return summed[None]


def solution(mesh):
    placed = (P("ka", None, "pw", None), P("ka", None, "pw", None), P(), P("pw"), P(), P())
    return jax.shard_map(
        local, mesh=mesh, in_specs=placed, out_specs=P("ka", "pw", None, None), check_vma=False
    )
```
